512 devices in a mesh: ctx: 64 (over z, y), tp: 8 (over x, core).
Axes of the slice: x: 4, y: 4, z: 16, core: 2. Of those that a mesh axis runs over, the one named last changes fastest.
Arguments:
- rotated_asking_vectors: bfloat16 [2, 2048, 64, 128], P(None, ('ctx', 'tp')), may hold values from -6 to 6
- rotated_match_vectors: bfloat16 [2, 2048, 8, 128], P(None, ('ctx', 'tp')), may hold values from -6 to 6
- content_vectors: bfloat16 [2, 2048, 8, 128], P(None, ('ctx', 'tp')), may hold values from -6 to 6
- result_cotangent: bfloat16 [2, 2048, 64, 128], P(None, ('ctx', 'tp')), may hold values from -6 to 6
Outputs:
- attended: bfloat16 [2, 2048, 64, 128], P(None, ('ctx', 'tp'))
- grad_query: bfloat16 [2, 2048, 64, 128], P(None, ('ctx', 'tp'))
- grad_key: bfloat16 [2, 2048, 8, 128], P(None, ('ctx', 'tp'))
- grad_value: bfloat16 [2, 2048, 8, 128], P(None, ('ctx', 'tp'))
The draws below stay inside these ranges and needn't reach their ends.
All inputs are finite; a program needn't handle non-finite values.
Results may differ from the reference program's by a relative error of at most 0.002.
Values may be sent and summed in bfloat16 or wider, within the bound.
No kernel may reach another device: no remote copies, remote signals or barrier semaphores. Data moves between devices by JAX's collectives and lax.ppermute only.
A program may use at most 64 MiB of HBM per device.

```python
import jax
import jax.numpy as jnp
from jax import lax

ASKING_HEAD_COUNT = 64
SHARED_HEAD_COUNT = 8
HEAD_WIDTH = 128
DEPTH_COUNT = 2
WINDOW_LENGTH = 2048
QUERIES_PER_SHARED = 8


def level_of(key, extent, cuts, least, top_value):
    loudness, own = 1.0, jax.random.fold_in(key, 6)
    for position, parts in cuts:
        steps = jnp.exp(jax.random.uniform(jax.random.fold_in(own, position), (parts,), jnp.float32, least / len(cuts), top_value / len(cuts)))
        loudness = loudness * jnp.repeat(steps, extent[position] // parts).reshape([-1 if axis == position else 1 for axis in range(len(extent))])
    return loudness


def noise(rng, shape, spread, reach, pieces=(), kind=jnp.bfloat16):
    result = spread * jax.random.normal(rng, shape, jnp.float32)
    if pieces:
        result = result * level_of(rng, shape, pieces, -0.22, 0.18)
    return jnp.clip(result, -reach, reach).astype(kind)


def setup_inputs(seed: int = 0) -> dict:
    key_list = jax.random.split(jax.random.key(seed), 5)
    return {
        "rotated_asking_vectors": noise(key_list[0], (DEPTH_COUNT, WINDOW_LENGTH, ASKING_HEAD_COUNT, HEAD_WIDTH), 1.0, 6.0, ((1, 512),)),
        "rotated_match_vectors": noise(key_list[1], (DEPTH_COUNT, WINDOW_LENGTH, SHARED_HEAD_COUNT, HEAD_WIDTH), 1.0, 6.0, ((1, 512),)),
        "content_vectors": noise(key_list[2], (DEPTH_COUNT, WINDOW_LENGTH, SHARED_HEAD_COUNT, HEAD_WIDTH), 1.0, 6.0, ((1, 512),)),
        "result_cotangent": noise(key_list[3], (DEPTH_COUNT, WINDOW_LENGTH, ASKING_HEAD_COUNT, HEAD_WIDTH), 1.0, 6.0, ((1, 512),)),
    }


def head_group(operands):
    query_group, key_group, value_group, grad_group = operands
    softmax_scale = HEAD_WIDTH ** -0.5
    places = jnp.arange(WINDOW_LENGTH, dtype=jnp.int32)
    causal_mask = places[None, :] <= places[:, None]
    scores = jnp.einsum("gid,jd->gij", query_group, key_group, precision=lax.Precision.HIGHEST) * softmax_scale
    scores = jnp.where(causal_mask[None], scores, -jnp.inf)
    highest = jnp.max(scores, axis=-1, keepdims=True)
    log_norm = highest + jnp.log(jnp.sum(jnp.exp(scores - highest), axis=-1, keepdims=True))
    probabilities = jnp.exp(scores - log_norm)
    attended = jnp.einsum("gij,jd->gid", probabilities, value_group, precision=lax.Precision.HIGHEST).astype(jnp.bfloat16)
    saved_out = lax.optimization_barrier(attended).astype(jnp.float32)
    row_delta = jnp.sum(grad_group * saved_out, axis=-1, keepdims=True)
    prob_grad = jnp.einsum("gid,jd->gij", grad_group, value_group, precision=lax.Precision.HIGHEST)
    dscore = probabilities * (prob_grad - row_delta)
    query_grad = softmax_scale * jnp.einsum("gij,jd->gid", dscore, key_group, precision=lax.Precision.HIGHEST)
    key_grad = softmax_scale * jnp.einsum("gij,gid->jd", dscore, query_group, precision=lax.Precision.HIGHEST)
    value_grad = jnp.einsum("gij,gid->jd", probabilities, grad_group, precision=lax.Precision.HIGHEST)
    return attended, query_grad.astype(jnp.bfloat16), key_grad.astype(jnp.bfloat16), value_grad.astype(jnp.bfloat16)


def reference(rotated_asking_vectors, rotated_match_vectors, content_vectors, result_cotangent):
    outputs = ([], [], [], [])
    for depth_position in range(DEPTH_COUNT):
        expanded_asking_vectors = rotated_asking_vectors[depth_position].astype(jnp.float32).reshape(WINDOW_LENGTH, SHARED_HEAD_COUNT, QUERIES_PER_SHARED, HEAD_WIDTH).transpose(1, 2, 0, 3)
        expanded_cotangent = result_cotangent[depth_position].astype(jnp.float32).reshape(WINDOW_LENGTH, SHARED_HEAD_COUNT, QUERIES_PER_SHARED, HEAD_WIDTH).transpose(1, 2, 0, 3)
        key_wide = rotated_match_vectors[depth_position].astype(jnp.float32).transpose(1, 0, 2)
        value_wide = content_vectors[depth_position].astype(jnp.float32).transpose(1, 0, 2)
        attended, query_grad, key_grad, value_grad = lax.map(head_group, (expanded_asking_vectors, key_wide, value_wide, expanded_cotangent))
        outputs[0].append(attended.transpose(2, 0, 1, 3).reshape(WINDOW_LENGTH, ASKING_HEAD_COUNT, HEAD_WIDTH))
        outputs[1].append(query_grad.transpose(2, 0, 1, 3).reshape(WINDOW_LENGTH, ASKING_HEAD_COUNT, HEAD_WIDTH))
        outputs[2].append(key_grad.transpose(1, 0, 2))
        outputs[3].append(value_grad.transpose(1, 0, 2))
    return (jnp.stack(outputs[0]), jnp.stack(outputs[1]), jnp.stack(outputs[2]), jnp.stack(outputs[3]))
```

```python
import functools
import math

import jax
import jax.numpy as jnp
from jax import lax
from jax.experimental import pallas as pl
from jax.experimental.pallas import tpu as pltpu
from jax.sharding import Mesh
from jax.sharding import PartitionSpec as P

AXES = ("z", "y", "x", "c")
PLANE = ("y", "x")
SLABS, PEERS = 16, 16
TOKENS, GROUP, WIDTH = 4, 8, 128
ROWS = SLABS * TOKENS * GROUP
KEYS = 2048
CHUNK = 256
TILE = 128
HIDDEN_SCORE = -1e30
SCALE = WIDTH**-0.5
SCALE_LOG2 = SCALE * math.log2(math.e)

NT = (((1,), (1,)), ((), ()))
NN = (((1,), (0,)), ((), ()))


def dot(a, b, dims=NN):
    return lax.dot_general(a, b, dims, preferred_element_type=jnp.float32)


def two_parts(value):
    high = value.astype(jnp.bfloat16)
    return high, (value - high.astype(jnp.float32)).astype(jnp.bfloat16)


def fold_rows(value, op):
    return op(value.reshape(value.shape[0] // 8, 8, value.shape[1]), axis=0)


def attention_kernel(
    place_ref,
    rows_ref,
    mine_ref,
    other_ref,
    out_ref,
    mine_grad_ref,
    other_grad_ref,
    query,
    cotangent,
    keys,
    values,
    keys_t,
    values_t,
    cotangent_t,
    scores,
    peak,
    total,
    attended_t,
    grad_query_t,
):
    core, place = place_ref[0], place_ref[1]
    query[...] = rows_ref[:, 0:32, :].reshape(ROWS, WIDTH)
    cotangent[...] = rows_ref[:, 32:64, :].reshape(ROWS, WIDTH)
    first_half = lax.broadcasted_iota(jnp.int32, (PEERS, 8, WIDTH), 1) < 4

    def sort_slab(z, carry):
        a = mine_ref[:, z].astype(jnp.float32)
        b = other_ref[:, z].astype(jnp.float32)
        key = jnp.where(first_half, a, pltpu.roll(b, 4, 1)).reshape(TILE, WIDTH)
        value = jnp.where(first_half, pltpu.roll(a, 4, 1), b).reshape(TILE, WIDTH)
        at = pl.ds(pl.multiple_of(z * TILE, TILE), TILE)
        keys[at, :] = key.astype(jnp.bfloat16)
        values[at, :] = value.astype(jnp.bfloat16)
        keys_t[:, at] = key.T.astype(jnp.bfloat16)
        values_t[:, at] = value.T.astype(jnp.bfloat16)
        return carry

    lax.fori_loop(0, SLABS, sort_slab, 0)
    cotangent_t[...] = cotangent[...].astype(jnp.float32).T
    peak[...] = jnp.full(peak.shape, HIDDEN_SCORE, jnp.float32)
    total[...] = jnp.zeros(total.shape, jnp.float32)
    attended_t[...] = jnp.zeros(attended_t.shape, jnp.float32)
    grad_query_t[...] = jnp.zeros(grad_query_t.shape, jnp.float32)

    def over_chunks(step):
        for b in range(ROWS // TILE):
            def body(i, carry, b=b):
                step(b * TILE, pl.multiple_of(b * 512 + i * CHUNK, CHUNK))
                return carry

            lax.fori_loop(0, 512 // CHUNK, body, 0)

    def score_step(low, first):
        at = pl.ds(first, CHUNK)
        s = dot(keys[at, :], query[low:, :], NT) * SCALE_LOG2
        key_at = first + lax.broadcasted_iota(jnp.int32, (CHUNK, TILE), 0)
        key_at = key_at ^ (4 * core)
        row = low + lax.broadcasted_iota(jnp.int32, (CHUNK, TILE), 1)
        row_at = (row // 32) * 128 + place * 8 + core * 4 + (row % 32) // 8
        near = jnp.where(key_at <= row_at, s[:, :TILE], HIDDEN_SCORE)
        scores[at, low : low + TILE] = near
        peak[:, low : low + TILE] = jnp.maximum(peak[:, low : low + TILE], fold_rows(near, jnp.max))
        if low + TILE < ROWS:
            far = s[:, TILE:]
            scores[at, low + TILE :] = far
            peak[:, low + TILE :] = jnp.maximum(peak[:, low + TILE :], fold_rows(far, jnp.max))

    over_chunks(score_step)
    peak[...] = jnp.broadcast_to(jnp.max(peak[...], axis=0, keepdims=True), peak.shape)

    def forward_step(low, first):
        at = pl.ds(first, CHUNK)
        p = jnp.exp2(scores[at, low:] - peak[0:1, low:])
        scores[at, low:] = p
        total[:, low:] += fold_rows(p, jnp.sum)
        high, rest = two_parts(p)
        v = values_t[:, at]
        attended_t[:, low:] += dot(v, high) + dot(v, rest)

    over_chunks(forward_step)
    inverse = 1.0 / jnp.sum(total[...], axis=0, keepdims=True)
    attended = (attended_t[...] * inverse).T.astype(jnp.bfloat16)
    out_ref[:, 0:32, :] = attended.reshape(SLABS, 32, WIDTH)
    delta = jnp.sum(attended.astype(jnp.float32).T * cotangent_t[...], axis=0, keepdims=True)
    total[...] = jnp.broadcast_to(inverse, total.shape)
    peak[...] = jnp.broadcast_to(delta, peak.shape)

    def backward_step(low, first):
        at = pl.ds(first, CHUNK)
        grad = dot(values[at, :], cotangent[low:, :], NT)
        p = scores[at, low:] * total[0:1, low:]
        p_high, p_rest = two_parts(p)
        d_high, d_rest = two_parts(p * (grad - peak[0:1, low:]))
        value_grad = dot(p_high, cotangent[low:, :]) + dot(p_rest, cotangent[low:, :])
        key_grad = SCALE * (dot(d_high, query[low:, :]) + dot(d_rest, query[low:, :]))
        k = keys_t[:, at]
        grad_query_t[:, low:] += dot(k, d_high) + dot(k, d_rest)
        slabs = CHUNK // TILE
        for n in range(slabs):
            kg = key_grad[n * TILE : (n + 1) * TILE].reshape(PEERS, 8, WIDTH)
            vg = value_grad[n * TILE : (n + 1) * TILE].reshape(PEERS, 8, WIDTH)
            z = first // TILE + n
            mine_grad_ref[:, z] = jnp.where(first_half, kg, pltpu.roll(vg, 4, 1))
            other_grad_ref[:, z] = jnp.where(first_half, pltpu.roll(kg, 4, 1), vg)

    over_chunks(backward_step)
    grad_query = (grad_query_t[...] * SCALE).T.astype(jnp.bfloat16)
    out_ref[:, 32:64, :] = grad_query.reshape(SLABS, 32, WIDTH)


def attention(place, rows, mine, other):
    bf, f32 = jnp.bfloat16, jnp.float32
    whole = pl.BlockSpec(memory_space=pltpu.VMEM)
    return pl.pallas_call(
        attention_kernel,
        out_shape=(
            jax.ShapeDtypeStruct((SLABS, 64, WIDTH), bf),
            jax.ShapeDtypeStruct((PEERS, SLABS, 8, WIDTH), f32),
            jax.ShapeDtypeStruct((PEERS, SLABS, 8, WIDTH), f32),
        ),
        in_specs=[pl.BlockSpec(memory_space=pltpu.SMEM), whole, whole, whole],
        out_specs=(whole, whole, whole),
        scratch_shapes=[
            pltpu.VMEM((ROWS, WIDTH), bf),
            pltpu.VMEM((ROWS, WIDTH), bf),
            pltpu.VMEM((KEYS, WIDTH), bf),
            pltpu.VMEM((KEYS, WIDTH), bf),
            pltpu.VMEM((WIDTH, KEYS), bf),
            pltpu.VMEM((WIDTH, KEYS), bf),
            pltpu.VMEM((WIDTH, ROWS), f32),
            pltpu.VMEM((KEYS, ROWS), f32),
            pltpu.VMEM((8, ROWS), f32),
            pltpu.VMEM((8, ROWS), f32),
            pltpu.VMEM((WIDTH, ROWS), f32),
            pltpu.VMEM((WIDTH, ROWS), f32),
        ],
        cost_estimate=pl.CostEstimate(
            flops=10 * 2 * KEYS * ROWS * WIDTH, bytes_accessed=4 << 20, transcendentals=KEYS * ROWS
        ),
        name="attention",
    )(place, rows, mine, other)


def by_pair(value, heads):
    value = value.reshape(2, TOKENS, 8, heads, WIDTH).transpose(0, 2, 1, 3, 4)
    return value.reshape(SLABS, TOKENS * heads, WIDTH)


def by_token(value, heads):
    value = value.reshape(2, 8, TOKENS, heads, WIDTH).transpose(0, 2, 1, 3, 4)
    return value.reshape(2, TOKENS, 8 * heads, WIDTH)


def on_device(query, key, value, cotangent):
    core = lax.axis_index("c")
    place = jnp.stack([core, lax.axis_index("y") * 4 + lax.axis_index("x")]).astype(jnp.int32)
    sent = jnp.concatenate(
        [by_pair(query, GROUP), by_pair(cotangent, GROUP), by_pair(key, 1), by_pair(value, 1)], axis=1
    )
    rows = lax.all_to_all(sent, "z", 0, 0)
    slab = jnp.broadcast_to(rows[:, 64:72, :][None], (PEERS, SLABS, 8, WIDTH))
    mine = lax.all_to_all(slab, PLANE, 0, 0)
    swap = [(0, 1), (1, 0)]
    other = lax.ppermute(mine, "c", swap)
    out, mine_grad, other_grad = attention(place, rows, mine, other)
    mine_grad = mine_grad + lax.ppermute(other_grad, "c", swap)
    parts = lax.all_to_all(mine_grad, PLANE, 0, 0)
    pair_grad = jnp.sum(parts, axis=0).astype(jnp.bfloat16)
    back = lax.all_to_all(jnp.concatenate([out, pair_grad], axis=1), "z", 0, 0)
    return (
        by_token(back[:, 0:32], GROUP),
        by_token(back[:, 32:64], GROUP),
        by_token(back[:, 64:68], 1),
        by_token(back[:, 68:72], 1),
    )


def solution(mesh):
    torus = Mesh(mesh.devices.reshape(16, 4, 4, 2), AXES)
    spec = P(None, AXES, None, None)
    return jax.shard_map(
        on_device, mesh=torus, in_specs=(spec,) * 4, out_specs=(spec,) * 4, check_vma=False
    )
```

```python
import functools
import math

import jax
import jax.numpy as jnp
from jax import lax
from jax.experimental import pallas as pl
from jax.experimental.pallas import tpu as pltpu
from jax.sharding import Mesh
from jax.sharding import PartitionSpec as P

AXES = ("z", "y", "x", "c")
PLANE = ("y", "x")
SLABS, PEERS = 16, 16
TOKENS, GROUP, WIDTH = 4, 8, 128
ROWS = SLABS * TOKENS * GROUP
KEYS = 2048
CHUNK = 256
TILE = 128
HIDDEN_SCORE = -1e30
SCALE = WIDTH**-0.5
SCALE_LOG2 = SCALE * math.log2(math.e)

NT = (((1,), (1,)), ((), ()))
NN = (((1,), (0,)), ((), ()))


def dot(a, b, dims=NN):
    return lax.dot_general(a, b, dims, preferred_element_type=jnp.float32)


def two_parts(value):
    high = value.astype(jnp.bfloat16)
    return high, (value - high.astype(jnp.float32)).astype(jnp.bfloat16)


def fold_rows(value, op):
    return op(value.reshape(value.shape[0] // 8, 8, value.shape[1]), axis=0)


def attention_kernel(
    place_ref,
    rows_ref,
    mine_ref,
    other_ref,
    out_ref,
    mine_grad_ref,
    other_grad_ref,
    query,
    cotangent,
    keys,
    values,
    keys_t,
    values_t,
    cotangent_t,
    scores,
    peak,
    total,
    attended_t,
    grad_query_t,
):
    core, place = place_ref[0], place_ref[1]
    query[...] = rows_ref[:, 0:32, :].reshape(ROWS, WIDTH)
    cotangent[...] = rows_ref[:, 32:64, :].reshape(ROWS, WIDTH)
    first_half = lax.broadcasted_iota(jnp.int32, (PEERS, 8, WIDTH), 1) < 4

    def sort_slab(z, carry):
        a = mine_ref[:, z].astype(jnp.float32)
        b = other_ref[:, z].astype(jnp.float32)
        key = jnp.where(first_half, a, pltpu.roll(b, 4, 1)).reshape(TILE, WIDTH)
        value = jnp.where(first_half, pltpu.roll(a, 4, 1), b).reshape(TILE, WIDTH)
        at = pl.ds(pl.multiple_of(z * TILE, TILE), TILE)
        keys[at, :] = key.astype(jnp.bfloat16)
        values[at, :] = value.astype(jnp.bfloat16)
        keys_t[:, at] = key.T.astype(jnp.bfloat16)
        values_t[:, at] = value.T.astype(jnp.bfloat16)
        return carry

    lax.fori_loop(0, SLABS, sort_slab, 0)
    cotangent_t[...] = cotangent[...].astype(jnp.float32).T
    peak[...] = jnp.full(peak.shape, HIDDEN_SCORE, jnp.float32)
    total[...] = jnp.zeros(total.shape, jnp.float32)
    attended_t[...] = jnp.zeros(attended_t.shape, jnp.float32)
    grad_query_t[...] = jnp.zeros(grad_query_t.shape, jnp.float32)

    def over_chunks(step):
        for b in range(ROWS // TILE):
            def body(i, carry, b=b):
                step(b * TILE, pl.multiple_of(b * 512 + i * CHUNK, CHUNK))
                return carry

            lax.fori_loop(0, 512 // CHUNK, body, 0)

    def score_step(low, first):
        at = pl.ds(first, CHUNK)
        s = dot(keys[at, :], query[low:, :], NT) * SCALE_LOG2
        key_at = first + lax.broadcasted_iota(jnp.int32, (CHUNK, TILE), 0)
        key_at = key_at ^ (4 * core)
        row = low + lax.broadcasted_iota(jnp.int32, (CHUNK, TILE), 1)
        row_at = (row // 32) * 128 + place * 8 + core * 4 + (row % 32) // 8
        near = jnp.where(key_at <= row_at, s[:, :TILE], HIDDEN_SCORE)
        scores[at, low : low + TILE] = near
        peak[:, low : low + TILE] = jnp.maximum(peak[:, low : low + TILE], fold_rows(near, jnp.max))
        if low + TILE < ROWS:
            far = s[:, TILE:]
            scores[at, low + TILE :] = far
            peak[:, low + TILE :] = jnp.maximum(peak[:, low + TILE :], fold_rows(far, jnp.max))

    over_chunks(score_step)
    peak[...] = jnp.broadcast_to(jnp.max(peak[...], axis=0, keepdims=True), peak.shape)

    def forward_step(low, first):
        at = pl.ds(first, CHUNK)
        p = jnp.exp2(scores[at, low:] - peak[0:1, low:])
        scores[at, low:] = p
        total[:, low:] += fold_rows(p, jnp.sum)
        high, rest = two_parts(p)
        v = values_t[:, at]
        attended_t[:, low:] += dot(v, high) + dot(v, rest)

    over_chunks(forward_step)
    inverse = 1.0 / jnp.sum(total[...], axis=0, keepdims=True)
    attended = (attended_t[...] * inverse).T.astype(jnp.bfloat16)
    out_ref[:, 0:32, :] = attended.reshape(SLABS, 32, WIDTH)
    delta = jnp.sum(attended.astype(jnp.float32).T * cotangent_t[...], axis=0, keepdims=True)
    total[...] = jnp.broadcast_to(inverse, total.shape)
    peak[...] = jnp.broadcast_to(delta, peak.shape)

    def backward_step(low, first):
        at = pl.ds(first, CHUNK)
        grad = dot(values[at, :], cotangent[low:, :], NT)
        p = scores[at, low:] * total[0:1, low:]
        p_high, p_rest = two_parts(p)
        d_high, d_rest = two_parts(p * (grad - peak[0:1, low:]))
        value_grad = dot(p_high, cotangent[low:, :]) + dot(p_rest, cotangent[low:, :])
        key_grad = SCALE * (dot(d_high, query[low:, :]) + dot(d_rest, query[low:, :]))
        k = keys_t[:, at]
        grad_query_t[:, low:] += dot(k, d_high) + dot(k, d_rest)
        slabs = CHUNK // TILE
        for n in range(slabs):
            kg = key_grad[n * TILE : (n + 1) * TILE].reshape(PEERS, 8, WIDTH)
            vg = value_grad[n * TILE : (n + 1) * TILE].reshape(PEERS, 8, WIDTH)
            z = first // TILE + n
            mine_grad_ref[:, z] = jnp.where(first_half, kg, pltpu.roll(vg, 4, 1))
            other_grad_ref[:, z] = jnp.where(first_half, pltpu.roll(kg, 4, 1), vg)

    over_chunks(backward_step)
    grad_query = (grad_query_t[...] * SCALE).T.astype(jnp.bfloat16)
    out_ref[:, 32:64, :] = grad_query.reshape(SLABS, 32, WIDTH)


def attention(place, rows, mine, other):
    bf, f32 = jnp.bfloat16, jnp.float32
    whole = pl.BlockSpec(memory_space=pltpu.VMEM)
    return pl.pallas_call(
        attention_kernel,
        out_shape=(
            jax.ShapeDtypeStruct((SLABS, 64, WIDTH), bf),
            jax.ShapeDtypeStruct((PEERS, SLABS, 8, WIDTH), f32),
            jax.ShapeDtypeStruct((PEERS, SLABS, 8, WIDTH), f32),
        ),
        in_specs=[pl.BlockSpec(memory_space=pltpu.SMEM), whole, whole, whole],
        out_specs=(whole, whole, whole),
        scratch_shapes=[
            pltpu.VMEM((ROWS, WIDTH), bf),
            pltpu.VMEM((ROWS, WIDTH), bf),
            pltpu.VMEM((KEYS, WIDTH), bf),
            pltpu.VMEM((KEYS, WIDTH), bf),
            pltpu.VMEM((WIDTH, KEYS), bf),
            pltpu.VMEM((WIDTH, KEYS), bf),
            pltpu.VMEM((WIDTH, ROWS), f32),
            pltpu.VMEM((KEYS, ROWS), f32),
            pltpu.VMEM((8, ROWS), f32),
            pltpu.VMEM((8, ROWS), f32),
            pltpu.VMEM((WIDTH, ROWS), f32),
            pltpu.VMEM((WIDTH, ROWS), f32),
        ],
        cost_estimate=pl.CostEstimate(
            flops=10 * 2 * KEYS * ROWS * WIDTH, bytes_accessed=4 << 20, transcendentals=KEYS * ROWS
        ),
        compiler_params=pltpu.CompilerParams(vmem_limit_bytes=24 << 20),
        name="attention",
    )(place, rows, mine, other)


def by_pair(value, heads):
    value = value.reshape(2, TOKENS, 8, heads, WIDTH).transpose(0, 2, 1, 3, 4)
    return value.reshape(SLABS, TOKENS * heads, WIDTH)


def by_token(value, heads):
    value = value.reshape(2, 8, TOKENS, heads, WIDTH).transpose(0, 2, 1, 3, 4)
    return value.reshape(2, TOKENS, 8 * heads, WIDTH)


def on_device(query, key, value, cotangent):
    core = lax.axis_index("c")
    place = jnp.stack([core, lax.axis_index("y") * 4 + lax.axis_index("x")]).astype(jnp.int32)
    sent = jnp.concatenate(
        [by_pair(query, GROUP), by_pair(cotangent, GROUP), by_pair(key, 1), by_pair(value, 1)], axis=1
    )
    rows = lax.all_to_all(sent, "z", 0, 0)
    slab = jnp.broadcast_to(rows[:, 64:72, :][None], (PEERS, SLABS, 8, WIDTH))
    mine = lax.all_to_all(slab, PLANE, 0, 0)
    swap = [(0, 1), (1, 0)]
    other = lax.ppermute(mine, "c", swap)
    out, mine_grad, other_grad = attention(place, rows, mine, other)
    mine_grad = mine_grad + lax.ppermute(other_grad, "c", swap)
    parts = lax.all_to_all(mine_grad, PLANE, 0, 0)
    pair_grad = jnp.sum(parts, axis=0).astype(jnp.bfloat16)
    back = lax.all_to_all(jnp.concatenate([out, pair_grad], axis=1), "z", 0, 0)
    return (
        by_token(back[:, 0:32], GROUP),
        by_token(back[:, 32:64], GROUP),
        by_token(back[:, 64:68], 1),
        by_token(back[:, 68:72], 1),
    )


def solution(mesh):
    torus = Mesh(mesh.devices.reshape(16, 4, 4, 2), AXES)
    spec = P(None, AXES, None, None)
    return jax.shard_map(
        on_device, mesh=torus, in_specs=(spec,) * 4, out_specs=(spec,) * 4, check_vma=False
    )
```

```python
import functools
import math

import jax
import jax.numpy as jnp
from jax import lax
from jax.experimental import pallas as pl
from jax.experimental.pallas import tpu as pltpu
from jax.sharding import Mesh
from jax.sharding import PartitionSpec as P

AXES = ("z", "y", "x", "c")
PLANE = ("y", "x")
SLABS, PEERS = 16, 16
TOKENS, GROUP, WIDTH = 4, 8, 128
ROWS = SLABS * TOKENS * GROUP
KEYS = 2048
CHUNK = 512
TILE = 128
HIDDEN_SCORE = -1e30
SCALE = WIDTH**-0.5
SCALE_LOG2 = SCALE * math.log2(math.e)

NT = (((1,), (1,)), ((), ()))
NN = (((1,), (0,)), ((), ()))


def dot(a, b, dims=NN):
    return lax.dot_general(a, b, dims, preferred_element_type=jnp.float32)


def two_parts(value):
    high = value.astype(jnp.bfloat16)
    return high, (value - high.astype(jnp.float32)).astype(jnp.bfloat16)


def fold_rows(value, op):
    return op(value.reshape(value.shape[0] // 8, 8, value.shape[1]), axis=0)


def attention_kernel(
    place_ref,
    rows_ref,
    mine_ref,
    other_ref,
    out_ref,
    mine_grad_ref,
    other_grad_ref,
    query,
    cotangent,
    keys,
    values,
    keys_t,
    values_t,
    cotangent_t,
    scores,
    peak,
    total,
    attended_t,
    grad_query_t,
):
    core, place = place_ref[0], place_ref[1]
    query[...] = rows_ref[:, 0:32, :].reshape(ROWS, WIDTH)
    cotangent[...] = rows_ref[:, 32:64, :].reshape(ROWS, WIDTH)
    first_half = lax.broadcasted_iota(jnp.int32, (PEERS, 8, WIDTH), 1) < 4

    def sort_slab(z, carry):
        a = mine_ref[:, z].astype(jnp.float32)
        b = other_ref[:, z].astype(jnp.float32)
        key = jnp.where(first_half, a, pltpu.roll(b, 4, 1)).reshape(TILE, WIDTH)
        value = jnp.where(first_half, pltpu.roll(a, 4, 1), b).reshape(TILE, WIDTH)
        at = pl.ds(pl.multiple_of(z * TILE, TILE), TILE)
        keys[at, :] = key.astype(jnp.bfloat16)
        values[at, :] = value.astype(jnp.bfloat16)
        keys_t[:, at] = key.T.astype(jnp.bfloat16)
        values_t[:, at] = value.T.astype(jnp.bfloat16)
        return carry

    lax.fori_loop(0, SLABS, sort_slab, 0, unroll=4)
    cotangent_t[...] = cotangent[...].astype(jnp.float32).T
    peak[...] = jnp.full(peak.shape, HIDDEN_SCORE, jnp.float32)
    total[...] = jnp.zeros(total.shape, jnp.float32)
    attended_t[...] = jnp.zeros(attended_t.shape, jnp.float32)
    grad_query_t[...] = jnp.zeros(grad_query_t.shape, jnp.float32)

    def over_chunks(step):
        for b in range(ROWS // TILE):
            def body(i, carry, b=b):
                step(b * TILE, pl.multiple_of(b * 512 + i * CHUNK, CHUNK))
                return carry

            lax.fori_loop(0, 512 // CHUNK, body, 0)

    def score_step(low, first):
        at = pl.ds(first, CHUNK)
        s = dot(keys[at, :], query[low:, :], NT) * SCALE_LOG2
        key_at = first + lax.broadcasted_iota(jnp.int32, (CHUNK, TILE), 0)
        key_at = key_at ^ (4 * core)
        row = low + lax.broadcasted_iota(jnp.int32, (CHUNK, TILE), 1)
        row_at = (row // 32) * 128 + place * 8 + core * 4 + (row % 32) // 8
        near = jnp.where(key_at <= row_at, s[:, :TILE], HIDDEN_SCORE)
        scores[at, low : low + TILE] = near
        peak[:, low : low + TILE] = jnp.maximum(peak[:, low : low + TILE], fold_rows(near, jnp.max))
        if low + TILE < ROWS:
            far = s[:, TILE:]
            scores[at, low + TILE :] = far
            peak[:, low + TILE :] = jnp.maximum(peak[:, low + TILE :], fold_rows(far, jnp.max))

    over_chunks(score_step)
    peak[...] = jnp.broadcast_to(jnp.max(peak[...], axis=0, keepdims=True), peak.shape)

    def forward_step(low, first):
        at = pl.ds(first, CHUNK)
        p = jnp.exp2(scores[at, low:] - peak[0:1, low:])
        scores[at, low:] = p
        total[:, low:] += fold_rows(p, jnp.sum)
        high, rest = two_parts(p)
        v = values_t[:, at]
        attended_t[:, low:] += dot(v, high) + dot(v, rest)

    over_chunks(forward_step)
    inverse = 1.0 / jnp.sum(total[...], axis=0, keepdims=True)
    attended = (attended_t[...] * inverse).T.astype(jnp.bfloat16)
    out_ref[:, 0:32, :] = attended.reshape(SLABS, 32, WIDTH)
    delta = jnp.sum(attended.astype(jnp.float32).T * cotangent_t[...], axis=0, keepdims=True)
    total[...] = jnp.broadcast_to(inverse, total.shape)
    peak[...] = jnp.broadcast_to(delta, peak.shape)

    def backward_step(low, first):
        at = pl.ds(first, CHUNK)
        grad = dot(values[at, :], cotangent[low:, :], NT)
        p = scores[at, low:] * total[0:1, low:]
        p_high, p_rest = two_parts(p)
        d_high, d_rest = two_parts(p * (grad - peak[0:1, low:]))
        value_grad = dot(p_high, cotangent[low:, :]) + dot(p_rest, cotangent[low:, :])
        key_grad = SCALE * (dot(d_high, query[low:, :]) + dot(d_rest, query[low:, :]))
        k = keys_t[:, at]
        grad_query_t[:, low:] += dot(k, d_high) + dot(k, d_rest)
        slabs = CHUNK // TILE
        for n in range(slabs):
            kg = key_grad[n * TILE : (n + 1) * TILE].reshape(PEERS, 8, WIDTH)
            vg = value_grad[n * TILE : (n + 1) * TILE].reshape(PEERS, 8, WIDTH)
            z = first // TILE + n
            mine_grad_ref[:, z] = jnp.where(first_half, kg, pltpu.roll(vg, 4, 1))
            other_grad_ref[:, z] = jnp.where(first_half, pltpu.roll(kg, 4, 1), vg)

    over_chunks(backward_step)
    grad_query = (grad_query_t[...] * SCALE).T.astype(jnp.bfloat16)
    out_ref[:, 32:64, :] = grad_query.reshape(SLABS, 32, WIDTH)


def attention(place, rows, mine, other):
    bf, f32 = jnp.bfloat16, jnp.float32
    whole = pl.BlockSpec(memory_space=pltpu.VMEM)
    return pl.pallas_call(
        attention_kernel,
        out_shape=(
            jax.ShapeDtypeStruct((SLABS, 64, WIDTH), bf),
            jax.ShapeDtypeStruct((PEERS, SLABS, 8, WIDTH), f32),
            jax.ShapeDtypeStruct((PEERS, SLABS, 8, WIDTH), f32),
        ),
        in_specs=[pl.BlockSpec(memory_space=pltpu.SMEM), whole, whole, whole],
        out_specs=(whole, whole, whole),
        scratch_shapes=[
            pltpu.VMEM((ROWS, WIDTH), bf),
            pltpu.VMEM((ROWS, WIDTH), bf),
            pltpu.VMEM((KEYS, WIDTH), bf),
            pltpu.VMEM((KEYS, WIDTH), bf),
            pltpu.VMEM((WIDTH, KEYS), bf),
            pltpu.VMEM((WIDTH, KEYS), bf),
            pltpu.VMEM((WIDTH, ROWS), f32),
            pltpu.VMEM((KEYS, ROWS), f32),
            pltpu.VMEM((8, ROWS), f32),
            pltpu.VMEM((8, ROWS), f32),
            pltpu.VMEM((WIDTH, ROWS), f32),
            pltpu.VMEM((WIDTH, ROWS), f32),
        ],
        cost_estimate=pl.CostEstimate(
            flops=10 * 2 * KEYS * ROWS * WIDTH, bytes_accessed=4 << 20, transcendentals=KEYS * ROWS
        ),
        compiler_params=pltpu.CompilerParams(vmem_limit_bytes=24 << 20),
        name="attention",
    )(place, rows, mine, other)


def by_pair(value, heads):
    value = value.reshape(2, TOKENS, 8, heads, WIDTH).transpose(0, 2, 1, 3, 4)
    return value.reshape(SLABS, TOKENS * heads, WIDTH)


def by_token(value, heads):
    value = value.reshape(2, 8, TOKENS, heads, WIDTH).transpose(0, 2, 1, 3, 4)
    return value.reshape(2, TOKENS, 8 * heads, WIDTH)


def on_device(query, key, value, cotangent):
    core = lax.axis_index("c")
    place = jnp.stack([core, lax.axis_index("y") * 4 + lax.axis_index("x")]).astype(jnp.int32)
    sent = jnp.concatenate(
        [by_pair(query, GROUP), by_pair(cotangent, GROUP), by_pair(key, 1), by_pair(value, 1)], axis=1
    )
    rows = lax.all_to_all(sent, "z", 0, 0)
    slab = jnp.broadcast_to(rows[:, 64:72, :][None], (PEERS, SLABS, 8, WIDTH))
    mine = lax.all_to_all(slab, PLANE, 0, 0)
    swap = [(0, 1), (1, 0)]
    other = lax.ppermute(mine, "c", swap)
    out, mine_grad, other_grad = attention(place, rows, mine, other)
    mine_grad = mine_grad + lax.ppermute(other_grad, "c", swap)
    parts = lax.all_to_all(mine_grad, PLANE, 0, 0)
    pair_grad = jnp.sum(parts, axis=0).astype(jnp.bfloat16)
    back = lax.all_to_all(jnp.concatenate([out, pair_grad], axis=1), "z", 0, 0)
    return (
        by_token(back[:, 0:32], GROUP),
        by_token(back[:, 32:64], GROUP),
        by_token(back[:, 64:68], 1),
        by_token(back[:, 68:72], 1),
    )


def solution(mesh):
    torus = Mesh(mesh.devices.reshape(16, 4, 4, 2), AXES)
    spec = P(None, AXES, None, None)
    return jax.shard_map(
        on_device, mesh=torus, in_specs=(spec,) * 4, out_specs=(spec,) * 4, check_vma=False
    )
```

```python
import functools
import math

import jax
import jax.numpy as jnp
from jax import lax
from jax.experimental import pallas as pl
from jax.experimental.pallas import tpu as pltpu
from jax.sharding import Mesh
from jax.sharding import PartitionSpec as P

AXES = ("z", "y", "x", "c")
PLANE = ("y", "x")
SLABS, PEERS = 16, 16
TOKENS, GROUP, WIDTH = 4, 8, 128
ROWS = SLABS * TOKENS * GROUP
KEYS = 2048
CHUNK = 512
TILE = 128
HIDDEN_SCORE = -1e30
FULL = 2.0**14
SCALE = WIDTH**-0.5
SCALE_LOG2 = SCALE * math.log2(math.e)

NT = (((1,), (1,)), ((), ()))
NN = (((1,), (0,)), ((), ()))


def dot(a, b, dims=NN):
    return lax.dot_general(a, b, dims, preferred_element_type=jnp.float32)


def two_parts(value):
    high = value.astype(jnp.bfloat16)
    return high, (value - high.astype(jnp.float32)).astype(jnp.bfloat16)


def fold_rows(value, op):
    return op(value.reshape(value.shape[0] // 8, 8, value.shape[1]), axis=0)


def attention_kernel(
    place_ref,
    rows_ref,
    mine_ref,
    other_ref,
    out_ref,
    mine_grad_ref,
    other_grad_ref,
    query,
    cotangent,
    keys,
    values,
    keys_t,
    values_t,
    cotangent_t,
    scores,
    peak,
    total,
    attended_t,
    grad_query_t,
    grad_peak,
):
    core, place = place_ref[0], place_ref[1]
    query[...] = rows_ref[:, 0:32, :].reshape(ROWS, WIDTH)
    cotangent[...] = rows_ref[:, 32:64, :].reshape(ROWS, WIDTH)
    first_half = lax.broadcasted_iota(jnp.int32, (PEERS, 8, WIDTH), 1) < 4

    def sort_slab(z, carry):
        a = mine_ref[:, z].astype(jnp.float32)
        b = other_ref[:, z].astype(jnp.float32)
        key = jnp.where(first_half, a, pltpu.roll(b, 4, 1)).reshape(TILE, WIDTH)
        value = jnp.where(first_half, pltpu.roll(a, 4, 1), b).reshape(TILE, WIDTH)
        at = pl.ds(pl.multiple_of(z * TILE, TILE), TILE)
        keys[at, :] = key.astype(jnp.bfloat16)
        values[at, :] = value.astype(jnp.bfloat16)
        keys_t[:, at] = key.T.astype(jnp.bfloat16)
        values_t[:, at] = value.T.astype(jnp.bfloat16)
        return carry

    lax.fori_loop(0, SLABS, sort_slab, 0, unroll=4)
    cotangent_t[...] = cotangent[...].astype(jnp.float32).T
    peak[...] = jnp.full(peak.shape, HIDDEN_SCORE, jnp.float32)
    total[...] = jnp.zeros(total.shape, jnp.float32)
    attended_t[...] = jnp.zeros(attended_t.shape, jnp.float32)
    grad_query_t[...] = jnp.zeros(grad_query_t.shape, jnp.float32)
    grad_peak[...] = jnp.zeros(grad_peak.shape, jnp.float32)

    def over_chunks(step):
        for b in range(ROWS // TILE):
            def body(i, carry, b=b):
                step(b * TILE, pl.multiple_of(b * 512 + i * CHUNK, CHUNK))
                return carry

            lax.fori_loop(0, 512 // CHUNK, body, 0)

    def score_step(low, first):
        at = pl.ds(first, CHUNK)
        s = dot(keys[at, :], query[low:, :], NT) * SCALE_LOG2
        key_at = first + lax.broadcasted_iota(jnp.int32, (CHUNK, TILE), 0)
        key_at = key_at ^ (4 * core)
        row = low + lax.broadcasted_iota(jnp.int32, (CHUNK, TILE), 1)
        row_at = (row // 32) * 128 + place * 8 + core * 4 + (row % 32) // 8
        near = jnp.where(key_at <= row_at, s[:, :TILE], HIDDEN_SCORE)
        scores[at, low : low + TILE] = near
        peak[:, low : low + TILE] = jnp.maximum(peak[:, low : low + TILE], fold_rows(near, jnp.max))
        if low + TILE < ROWS:
            far = s[:, TILE:]
            scores[at, low + TILE :] = far
            peak[:, low + TILE :] = jnp.maximum(peak[:, low + TILE :], fold_rows(far, jnp.max))

    over_chunks(score_step)
    peak[...] = jnp.broadcast_to(jnp.max(peak[...], axis=0, keepdims=True), peak.shape)

    def forward_step(low, first):
        at = pl.ds(first, CHUNK)
        p = jnp.exp2(scores[at, low:] - peak[0:1, low:])
        scores[at, low:] = p
        total[:, low:] += fold_rows(p, jnp.sum)
        high, rest = two_parts(p)
        v = values_t[:, at]
        attended_t[:, low:] += dot(v, high) + dot(v, rest)

    over_chunks(forward_step)
    inverse = 1.0 / jnp.sum(total[...], axis=0, keepdims=True)
    attended = (attended_t[...] * inverse).T.astype(jnp.bfloat16)
    out_ref[:, 0:32, :] = attended.reshape(SLABS, 32, WIDTH)
    delta = jnp.sum(attended.astype(jnp.float32).T * cotangent_t[...], axis=0, keepdims=True)
    total[...] = jnp.broadcast_to(inverse, total.shape)
    peak[...] = jnp.broadcast_to(delta, peak.shape)

    def backward_step(low, first):
        at = pl.ds(first, CHUNK)
        grad = dot(values[at, :], cotangent[low:, :], NT)
        p = scores[at, low:] * total[0:1, low:]
        p_high, p_rest = two_parts(p)
        d_high, d_rest = two_parts(p * (grad - peak[0:1, low:]))
        value_grad = dot(p_high, cotangent[low:, :]) + dot(p_rest, cotangent[low:, :])
        key_grad = SCALE * (dot(d_high, query[low:, :]) + dot(d_rest, query[low:, :]))
        k = keys_t[:, at]
        grad_query_t[:, low:] += dot(k, d_high) + dot(k, d_rest)
        both = jnp.maximum(jnp.abs(key_grad), jnp.abs(value_grad))
        grad_peak[...] = jnp.maximum(grad_peak[...], fold_rows(both, jnp.max))
        slabs = CHUNK // TILE
        for n in range(slabs):
            kg = key_grad[n * TILE : (n + 1) * TILE].reshape(PEERS, 8, WIDTH)
            vg = value_grad[n * TILE : (n + 1) * TILE].reshape(PEERS, 8, WIDTH)
            z = first // TILE + n
            mine_grad_ref[:, z] = jnp.where(first_half, kg, pltpu.roll(vg, 4, 1))
            other_grad_ref[:, z] = jnp.where(first_half, pltpu.roll(kg, 4, 1), vg)

    over_chunks(backward_step)
    grad_query = (grad_query_t[...] * SCALE).T.astype(jnp.bfloat16)
    out_ref[:, 32:64, :] = grad_query.reshape(SLABS, 32, WIDTH)
    mine_grad_ref[:, SLABS] = jnp.full((PEERS, 8, WIDTH), jnp.max(grad_peak[...]), jnp.float32)
    other_grad_ref[:, SLABS] = jnp.full((PEERS, 8, WIDTH), jnp.max(grad_peak[...]), jnp.float32)


def attention(place, rows, mine, other):
    bf, f32 = jnp.bfloat16, jnp.float32
    whole = pl.BlockSpec(memory_space=pltpu.VMEM)
    return pl.pallas_call(
        attention_kernel,
        out_shape=(
            jax.ShapeDtypeStruct((SLABS, 64, WIDTH), bf),
            jax.ShapeDtypeStruct((PEERS, SLABS + 1, 8, WIDTH), f32),
            jax.ShapeDtypeStruct((PEERS, SLABS + 1, 8, WIDTH), f32),
        ),
        in_specs=[pl.BlockSpec(memory_space=pltpu.SMEM), whole, whole, whole],
        out_specs=(whole, whole, whole),
        scratch_shapes=[
            pltpu.VMEM((ROWS, WIDTH), bf),
            pltpu.VMEM((ROWS, WIDTH), bf),
            pltpu.VMEM((KEYS, WIDTH), bf),
            pltpu.VMEM((KEYS, WIDTH), bf),
            pltpu.VMEM((WIDTH, KEYS), bf),
            pltpu.VMEM((WIDTH, KEYS), bf),
            pltpu.VMEM((WIDTH, ROWS), f32),
            pltpu.VMEM((KEYS, ROWS), f32),
            pltpu.VMEM((8, ROWS), f32),
            pltpu.VMEM((8, ROWS), f32),
            pltpu.VMEM((WIDTH, ROWS), f32),
            pltpu.VMEM((WIDTH, ROWS), f32),
            pltpu.VMEM((8, WIDTH), f32),
        ],
        cost_estimate=pl.CostEstimate(
            flops=10 * 2 * KEYS * ROWS * WIDTH, bytes_accessed=4 << 20, transcendentals=KEYS * ROWS
        ),
        compiler_params=pltpu.CompilerParams(vmem_limit_bytes=24 << 20),
        name="attention",
    )(place, rows, mine, other)


def fourth(root):
    square = root.astype(jnp.float32) ** 2
    return square * square


def by_pair(value, heads):
    value = value.reshape(2, TOKENS, 8, heads, WIDTH).transpose(0, 2, 1, 3, 4)
    return value.reshape(SLABS, TOKENS * heads, WIDTH)


def by_token(value, heads):
    value = value.reshape(2, 8, TOKENS, heads, WIDTH).transpose(0, 2, 1, 3, 4)
    return value.reshape(2, TOKENS, 8 * heads, WIDTH)


def on_device(query, key, value, cotangent):
    core = lax.axis_index("c")
    place = jnp.stack([core, lax.axis_index("y") * 4 + lax.axis_index("x")]).astype(jnp.int32)
    sent = jnp.concatenate(
        [by_pair(query, GROUP), by_pair(cotangent, GROUP), by_pair(key, 1), by_pair(value, 1)], axis=1
    )
    rows = lax.all_to_all(sent, "z", 0, 0)
    slab = jnp.broadcast_to(rows[:, 64:72, :][None], (PEERS, SLABS, 8, WIDTH))
    mine = lax.all_to_all(slab, PLANE, 0, 0)
    swap = [(0, 1), (1, 0)]
    other = lax.ppermute(mine, "c", swap)
    out, mine_grad, other_grad = attention(place, rows, mine, other)
    swapped = lax.ppermute(other_grad, "c", swap)
    total = mine_grad + swapped
    root = jnp.sqrt(jnp.sqrt(jnp.maximum(total[:, SLABS:], 1e-15)))
    root = lax.reduce_precision(root, exponent_bits=5, mantissa_bits=10)
    last = lax.broadcasted_iota(jnp.int32, total.shape, 1) == SLABS
    sent = jnp.where(last, root, total * (FULL / fourth(root))).astype(jnp.float16)
    parts = lax.all_to_all(sent, PLANE, 0, 0)
    scales = fourth(parts[:, SLABS:]) * (1.0 / FULL)
    pair_grad = jnp.sum(parts[:, :SLABS].astype(jnp.float32) * scales, axis=0).astype(jnp.bfloat16)
    back = lax.all_to_all(jnp.concatenate([out, pair_grad], axis=1), "z", 0, 0)
    return (
        by_token(back[:, 0:32], GROUP),
        by_token(back[:, 32:64], GROUP),
        by_token(back[:, 64:68], 1),
        by_token(back[:, 68:72], 1),
    )


def solution(mesh):
    torus = Mesh(mesh.devices.reshape(16, 4, 4, 2), AXES)
    spec = P(None, AXES, None, None)
    return jax.shard_map(
        on_device, mesh=torus, in_specs=(spec,) * 4, out_specs=(spec,) * 4, check_vma=False
    )
```

```python
import functools
import math

import jax
import jax.numpy as jnp
from jax import lax
from jax.experimental import pallas as pl
from jax.experimental.pallas import tpu as pltpu
from jax.sharding import Mesh
from jax.sharding import PartitionSpec as P

AXES = ("z", "y", "x", "c")
PLANE = ("y", "x")
SLABS, PEERS = 16, 16
TOKENS, GROUP, WIDTH = 4, 8, 128
ROWS = SLABS * TOKENS * GROUP
KEYS = 2048
CHUNK = 512
TILE = 128
HIDDEN_SCORE = -1e30
FULL = 2.0**14
SCALE = WIDTH**-0.5
SCALE_LOG2 = SCALE * math.log2(math.e)

NT = (((1,), (1,)), ((), ()))
NN = (((1,), (0,)), ((), ()))


def dot(a, b, dims=NN):
    return lax.dot_general(a, b, dims, preferred_element_type=jnp.float32)


def two_parts(value):
    high = value.astype(jnp.bfloat16)
    return high, (value - high.astype(jnp.float32)).astype(jnp.bfloat16)


def fold_rows(value, op):
    return op(value.reshape(value.shape[0] // 8, 8, value.shape[1]), axis=0)


def attention_kernel(
    place_ref,
    rows_ref,
    mine_ref,
    other_ref,
    out_ref,
    mine_grad_ref,
    other_grad_ref,
    query,
    cotangent,
    keys,
    values,
    keys_t,
    values_t,
    cotangent_t,
    scores,
    peak,
    total,
    attended_t,
    grad_query_t,
    grad_peak,
):
    core, place = place_ref[0], place_ref[1]
    query[...] = rows_ref[:, 0:32, :].reshape(ROWS, WIDTH)
    cotangent[...] = rows_ref[:, 32:64, :].reshape(ROWS, WIDTH)
    first_half = lax.broadcasted_iota(jnp.int32, (PEERS, 8, WIDTH), 1) < 4

    def sort_slab(z, carry):
        a = mine_ref[:, z].astype(jnp.float32)
        b = other_ref[:, z].astype(jnp.float32)
        key = jnp.where(first_half, a, pltpu.roll(b, 4, 1)).reshape(TILE, WIDTH)
        value = jnp.where(first_half, pltpu.roll(a, 4, 1), b).reshape(TILE, WIDTH)
        at = pl.ds(pl.multiple_of(z * TILE, TILE), TILE)
        keys[at, :] = key.astype(jnp.bfloat16)
        values[at, :] = value.astype(jnp.bfloat16)
        keys_t[:, at] = key.T.astype(jnp.bfloat16)
        values_t[:, at] = value.T.astype(jnp.bfloat16)
        return carry

    lax.fori_loop(0, SLABS, sort_slab, 0, unroll=4)
    cotangent_t[...] = cotangent[...].astype(jnp.float32).T
    peak[...] = jnp.full(peak.shape, HIDDEN_SCORE, jnp.float32)
    total[...] = jnp.zeros(total.shape, jnp.float32)
    attended_t[...] = jnp.zeros(attended_t.shape, jnp.float32)
    grad_query_t[...] = jnp.zeros(grad_query_t.shape, jnp.float32)
    grad_peak[...] = jnp.zeros(grad_peak.shape, jnp.float32)

    def over_chunks(step):
        for b in range(ROWS // TILE):
            def body(i, carry, b=b):
                step(b * TILE, pl.multiple_of(b * 512 + i * CHUNK, CHUNK))
                return carry

            lax.fori_loop(0, 512 // CHUNK, body, 0)

    def score_step(low, first):
        at = pl.ds(first, CHUNK)
        s = dot(keys[at, :], query[low:, :], NT) * SCALE_LOG2
        key_at = first + lax.broadcasted_iota(jnp.int32, (CHUNK, TILE), 0)
        key_at = key_at ^ (4 * core)
        row = low + lax.broadcasted_iota(jnp.int32, (CHUNK, TILE), 1)
        row_at = (row // 32) * 128 + place * 8 + core * 4 + (row % 32) // 8
        near = jnp.where(key_at <= row_at, s[:, :TILE], HIDDEN_SCORE)
        scores[at, low : low + TILE] = near
        peak[:, low : low + TILE] = jnp.maximum(peak[:, low : low + TILE], fold_rows(near, jnp.max))
        if low + TILE < ROWS:
            far = s[:, TILE:]
            scores[at, low + TILE :] = far
            peak[:, low + TILE :] = jnp.maximum(peak[:, low + TILE :], fold_rows(far, jnp.max))

    over_chunks(score_step)
    peak[...] = jnp.broadcast_to(jnp.max(peak[...], axis=0, keepdims=True), peak.shape)

    def forward_step(low, first):
        at = pl.ds(first, CHUNK)
        p = jnp.exp2(scores[at, low:] - peak[0:1, low:])
        scores[at, low:] = p
        total[:, low:] += fold_rows(p, jnp.sum)
        high, rest = two_parts(p)
        v = values_t[:, at]
        attended_t[:, low:] += dot(v, high) + dot(v, rest)

    over_chunks(forward_step)
    inverse = 1.0 / jnp.sum(total[...], axis=0, keepdims=True)
    attended = (attended_t[...] * inverse).T.astype(jnp.bfloat16)
    out_ref[:, 0:32, :] = attended.reshape(SLABS, 32, WIDTH)
    delta = jnp.sum(attended.astype(jnp.float32).T * cotangent_t[...], axis=0, keepdims=True)
    total[...] = jnp.broadcast_to(inverse, total.shape)
    peak[...] = jnp.broadcast_to(delta, peak.shape)

    def backward_step(low, first):
        at = pl.ds(first, CHUNK)
        grad = dot(values[at, :], cotangent[low:, :], NT)
        p = scores[at, low:] * total[0:1, low:]
        p_high, p_rest = two_parts(p)
        d_high, d_rest = two_parts(p * (grad - peak[0:1, low:]))
        value_grad = dot(p_high, cotangent[low:, :]) + dot(p_rest, cotangent[low:, :])
        key_grad = SCALE * (dot(d_high, query[low:, :]) + dot(d_rest, query[low:, :]))
        k = keys_t[:, at]
        grad_query_t[:, low:] += dot(k, d_high) + dot(k, d_rest)
        both = jnp.maximum(jnp.abs(key_grad), jnp.abs(value_grad))
        grad_peak[...] = jnp.maximum(grad_peak[...], fold_rows(both, jnp.max))
        slabs = CHUNK // TILE
        for n in range(slabs):
            kg = key_grad[n * TILE : (n + 1) * TILE].reshape(PEERS, 8, WIDTH)
            vg = value_grad[n * TILE : (n + 1) * TILE].reshape(PEERS, 8, WIDTH)
            z = first // TILE + n
            mine_grad_ref[:, z] = jnp.where(first_half, kg, pltpu.roll(vg, 4, 1))
            other_grad_ref[:, z] = jnp.where(first_half, pltpu.roll(kg, 4, 1), vg)

    over_chunks(backward_step)
    grad_query = (grad_query_t[...] * SCALE).T.astype(jnp.bfloat16)
    out_ref[:, 32:64, :] = grad_query.reshape(SLABS, 32, WIDTH)
    mine_grad_ref[:, SLABS] = jnp.full((PEERS, 8, WIDTH), jnp.max(grad_peak[...]), jnp.float32)
    other_grad_ref[:, SLABS] = jnp.full((PEERS, 8, WIDTH), jnp.max(grad_peak[...]), jnp.float32)


def attention(place, rows, mine, other):
    bf, f32 = jnp.bfloat16, jnp.float32
    whole = pl.BlockSpec(memory_space=pltpu.VMEM)
    return pl.pallas_call(
        attention_kernel,
        out_shape=(
            jax.ShapeDtypeStruct((SLABS, 64, WIDTH), bf),
            jax.ShapeDtypeStruct((PEERS, SLABS + 1, 8, WIDTH), f32),
            jax.ShapeDtypeStruct((PEERS, SLABS + 1, 8, WIDTH), f32),
        ),
        in_specs=[pl.BlockSpec(memory_space=pltpu.SMEM), whole, whole, whole],
        out_specs=(whole, whole, whole),
        scratch_shapes=[
            pltpu.VMEM((ROWS, WIDTH), bf),
            pltpu.VMEM((ROWS, WIDTH), bf),
            pltpu.VMEM((KEYS, WIDTH), bf),
            pltpu.VMEM((KEYS, WIDTH), bf),
            pltpu.VMEM((WIDTH, KEYS), bf),
            pltpu.VMEM((WIDTH, KEYS), bf),
            pltpu.VMEM((WIDTH, ROWS), f32),
            pltpu.VMEM((KEYS, ROWS), f32),
            pltpu.VMEM((8, ROWS), f32),
            pltpu.VMEM((8, ROWS), f32),
            pltpu.VMEM((WIDTH, ROWS), f32),
            pltpu.VMEM((WIDTH, ROWS), f32),
            pltpu.VMEM((8, WIDTH), f32),
        ],
        cost_estimate=pl.CostEstimate(
            flops=10 * 2 * KEYS * ROWS * WIDTH, bytes_accessed=4 << 20, transcendentals=KEYS * ROWS
        ),
        compiler_params=pltpu.CompilerParams(vmem_limit_bytes=24 << 20),
        name="attention",
    )(place, rows, mine, other)


def fourth(root):
    square = root.astype(jnp.float32) ** 2
    return square * square


def pack_kernel(query_ref, key_ref, value_ref, cotangent_ref, out_ref, narrow, pairs, wide_done, narrow_done):
    small = [
        pltpu.make_async_copy(source, narrow.at[n], narrow_done.at[n])
        for n, source in enumerate((key_ref, value_ref))
    ]
    for copy in small:
        copy.start()
    large = []
    for layer in range(2):
        for token in range(TOKENS):
            for n, source in enumerate((query_ref, cotangent_ref)):
                large.append(
                    pltpu.make_async_copy(
                        source.at[layer, token],
                        out_ref.at[pl.ds(layer * 8, 8), n * TOKENS + token],
                        wide_done.at[n, layer, token],
                    )
                )
    for copy in large:
        copy.start()
    for copy in small:
        copy.wait()
    for layer in range(2):
        for n in range(2):
            pairs[layer, n * TOKENS : (n + 1) * TOKENS] = narrow[n, layer].astype(jnp.float32)
        for group in range(8):
            out_ref[layer * 8 + group, 8] = pairs[layer, :, group, :].astype(jnp.bfloat16)
    for copy in large:
        copy.wait()


def pack(query, key, value, cotangent):
    far = pl.BlockSpec(memory_space=pltpu.HBM)
    by_group = (2, TOKENS, 8, GROUP, WIDTH)
    arrays = (query.reshape(by_group), key, value, cotangent.reshape(by_group))
    packed = pl.pallas_call(
        pack_kernel,
        out_shape=jax.ShapeDtypeStruct((SLABS, 9, 8, WIDTH), jnp.bfloat16),
        in_specs=[far] * 4,
        out_specs=pl.BlockSpec(memory_space=pltpu.VMEM),
        scratch_shapes=[
            pltpu.VMEM((2, 2, TOKENS, 8, WIDTH), jnp.bfloat16),
            pltpu.VMEM((2, 8, 8, WIDTH), jnp.float32),
            pltpu.SemaphoreType.DMA((2, 2, TOKENS)),
            pltpu.SemaphoreType.DMA((2,)),
        ],
        compiler_params=pltpu.CompilerParams(vmem_limit_bytes=4 << 20),
        name="pack",
    )(*[pltpu.with_memory_space_constraint(a, pltpu.HBM) for a in arrays])
    return packed.reshape(SLABS, 72, WIDTH)


def by_token(value, heads):
    value = value.reshape(2, 8, TOKENS, heads, WIDTH).transpose(0, 2, 1, 3, 4)
    return value.reshape(2, TOKENS, 8 * heads, WIDTH)


def on_device(query, key, value, cotangent):
    core = lax.axis_index("c")
    place = jnp.stack([core, lax.axis_index("y") * 4 + lax.axis_index("x")]).astype(jnp.int32)
    rows = lax.all_to_all(pack(query, key, value, cotangent), "z", 0, 0)
    slab = jnp.broadcast_to(rows[:, 64:72, :][None], (PEERS, SLABS, 8, WIDTH))
    mine = lax.all_to_all(slab, PLANE, 0, 0)
    swap = [(0, 1), (1, 0)]
    other = lax.ppermute(mine, "c", swap)
    out, mine_grad, other_grad = attention(place, rows, mine, other)
    swapped = lax.ppermute(other_grad, "c", swap)
    total = mine_grad + swapped
    root = jnp.sqrt(jnp.sqrt(jnp.maximum(total[:, SLABS:], 1e-15)))
    root = lax.reduce_precision(root, exponent_bits=5, mantissa_bits=10)
    last = lax.broadcasted_iota(jnp.int32, total.shape, 1) == SLABS
    sent = jnp.where(last, root, total * (FULL / fourth(root))).astype(jnp.float16)
    parts = lax.all_to_all(sent, PLANE, 0, 0)
    scales = fourth(parts[:, SLABS:]) * (1.0 / FULL)
    pair_grad = jnp.sum(parts[:, :SLABS].astype(jnp.float32) * scales, axis=0).astype(jnp.bfloat16)
    back = lax.all_to_all(jnp.concatenate([out, pair_grad], axis=1), "z", 0, 0)
    return (
        by_token(back[:, 0:32], GROUP),
        by_token(back[:, 32:64], GROUP),
        by_token(back[:, 64:68], 1),
        by_token(back[:, 68:72], 1),
    )


def solution(mesh):
    torus = Mesh(mesh.devices.reshape(16, 4, 4, 2), AXES)
    spec = P(None, AXES, None, None)
    return jax.shard_map(
        on_device, mesh=torus, in_specs=(spec,) * 4, out_specs=(spec,) * 4, check_vma=False
    )
```

```python
import functools
import math

import jax
import jax.numpy as jnp
from jax import lax
from jax.experimental import pallas as pl
from jax.experimental.pallas import tpu as pltpu
from jax.sharding import Mesh
from jax.sharding import PartitionSpec as P

AXES = ("z", "y", "x", "c")
PLANE = ("y", "x")
SLABS, PEERS = 16, 16
TOKENS, GROUP, WIDTH = 4, 8, 128
ROWS = SLABS * TOKENS * GROUP
KEYS = 2048
CHUNK = 256
TILE = 128
HIDDEN_SCORE = -1e30
FULL = 2.0**14
SCALE = WIDTH**-0.5
SCALE_LOG2 = SCALE * math.log2(math.e)

NT = (((1,), (1,)), ((), ()))
NN = (((1,), (0,)), ((), ()))


def dot(a, b, dims=NN):
    return lax.dot_general(a, b, dims, preferred_element_type=jnp.float32)


def two_parts(value):
    high = value.astype(jnp.bfloat16)
    return high, (value - high.astype(jnp.float32)).astype(jnp.bfloat16)


def fold_rows(value, op):
    return op(value.reshape(value.shape[0] // 8, 8, value.shape[1]), axis=0)


def sort_half(half_ref, keys, values, keys_t, values_t):
    first = lax.broadcasted_iota(jnp.int32, (PEERS // 2, 8, WIDTH), 1) < 4

    def step(n, carry):
        sorted_keys, sorted_values = [], []
        for slab in range(2):
            even = half_ref[:, 0, 2 * n + slab].astype(jnp.float32)
            odd = half_ref[:, 1, 2 * n + slab].astype(jnp.float32)
            sorted_keys.append(jnp.where(first, even, pltpu.roll(odd, 4, 1)).reshape(64, WIDTH))
            sorted_values.append(jnp.where(first, pltpu.roll(even, 4, 1), odd).reshape(64, WIDTH))
        key, value = jnp.concatenate(sorted_keys, axis=0), jnp.concatenate(sorted_values, axis=0)
        at = pl.ds(pl.multiple_of(n * TILE, TILE), TILE)
        keys[at, :] = key.astype(jnp.bfloat16)
        values[at, :] = value.astype(jnp.bfloat16)
        keys_t[:, at] = key.T.astype(jnp.bfloat16)
        values_t[:, at] = value.T.astype(jnp.bfloat16)
        return carry

    lax.fori_loop(0, SLABS // 2, step, 0, unroll=4)


def chunks():
    for b in range(ROWS // TILE):
        yield b * TILE, slice(b * CHUNK, (b + 1) * CHUNK)


def score_half(keys, query, scores, peak, core, place, key_core):
    for low, at in chunks():
        s = dot(keys[at, :], query[low:, :], NT) * SCALE_LOG2
        key = at.start + lax.broadcasted_iota(jnp.int32, (CHUNK, TILE), 0)
        key_at = (key // 64) * 128 + ((key % 64) // 4) * 8 + key_core * 4 + key % 4
        row = low + lax.broadcasted_iota(jnp.int32, (CHUNK, TILE), 1)
        row_at = (row // 32) * 128 + place * 8 + core * 4 + (row % 32) // 8
        near = jnp.where(key_at <= row_at, s[:, :TILE], HIDDEN_SCORE)
        scores[at, low : low + TILE] = near
        peak[:, low : low + TILE] = jnp.maximum(peak[:, low : low + TILE], fold_rows(near, jnp.max))
        if low + TILE < ROWS:
            far = s[:, TILE:]
            scores[at, low + TILE :] = far
            peak[:, low + TILE :] = jnp.maximum(peak[:, low + TILE :], fold_rows(far, jnp.max))


def forward_half(scores, weights, values_t, peak, total, attended_t):
    for low, at in chunks():
        p = jnp.exp2(scores[at, low:] - peak[0:1, low:])
        weights[at, low:] = p
        total[:, low:] += fold_rows(p, jnp.sum)
        high, rest = two_parts(p)
        v = values_t[:, at]
        attended_t[:, low:] += dot(v, high) + dot(v, rest)


def backward_half(query, cotangent, values, keys_t, weights, inverse, delta, grad_query_t, grad_ref, grad_peak):
    first = lax.broadcasted_iota(jnp.int32, (PEERS // 2, 8, WIDTH), 1) < 4
    grad_peak[...] = jnp.zeros(grad_peak.shape, jnp.float32)
    for low, at in chunks():
        grad = dot(values[at, :], cotangent[low:, :], NT)
        p = weights[at, low:] * inverse[0:1, low:]
        p_high, p_rest = two_parts(p)
        d_high, d_rest = two_parts(p * (grad - delta[0:1, low:]))
        value_grad = dot(p_high, cotangent[low:, :]) + dot(p_rest, cotangent[low:, :])
        key_grad = SCALE * (dot(d_high, query[low:, :]) + dot(d_rest, query[low:, :]))
        k = keys_t[:, at]
        grad_query_t[:, low:] += dot(k, d_high) + dot(k, d_rest)
        both = jnp.maximum(jnp.abs(key_grad), jnp.abs(value_grad))
        grad_peak[...] = jnp.maximum(grad_peak[...], fold_rows(both, jnp.max))
        for n in range(CHUNK // 64):
            kg = key_grad[n * 64 : (n + 1) * 64].reshape(PEERS // 2, 8, WIDTH)
            vg = value_grad[n * 64 : (n + 1) * 64].reshape(PEERS // 2, 8, WIDTH)
            slab = at.start // 64 + n
            grad_ref[:, 0, slab] = jnp.where(first, kg, pltpu.roll(vg, 4, 1))
            grad_ref[:, 1, slab] = jnp.where(first, pltpu.roll(kg, 4, 1), vg)
    grad_ref[:, :, SLABS] = jnp.full((PEERS // 2, 2, 8, WIDTH), jnp.max(grad_peak[...]), jnp.float32)


def first_kernel(
    place_ref, rows_ref, mine_ref, query, cotangent, cotangent_t, keys, values, keys_t, values_t, scores, peak
):
    query[...] = rows_ref[:, 0:32, :].reshape(ROWS, WIDTH)
    cotangent[...] = rows_ref[:, 32:64, :].reshape(ROWS, WIDTH)
    sort_half(mine_ref, keys, values, keys_t, values_t)
    cotangent_t[...] = cotangent[...].astype(jnp.float32).T
    peak[...] = jnp.full(peak.shape, HIDDEN_SCORE, jnp.float32)
    score_half(keys, query, scores, peak, place_ref[0], place_ref[1], place_ref[0])


def second_kernel(
    place_ref,
    other_ref,
    query,
    cotangent,
    cotangent_t,
    mine_values_t,
    mine_scores,
    mine_peak,
    attended_ref,
    grad_ref,
    mine_weights,
    inverse,
    delta,
    grad_query_t,
    keys,
    values,
    keys_t,
    values_t,
    scores,
    peak,
    total,
    attended_t,
    grad_peak,
):
    sort_half(other_ref, keys, values, keys_t, values_t)
    peak[...] = mine_peak[...]
    score_half(keys, query, scores, peak, place_ref[0], place_ref[1], 1 - place_ref[0])
    peak[...] = jnp.broadcast_to(jnp.max(peak[...], axis=0, keepdims=True), peak.shape)
    total[...] = jnp.zeros(total.shape, jnp.float32)
    attended_t[...] = jnp.zeros(attended_t.shape, jnp.float32)
    forward_half(mine_scores, mine_weights, mine_values_t, peak, total, attended_t)
    forward_half(scores, scores, values_t, peak, total, attended_t)
    scale = 1.0 / jnp.sum(total[...], axis=0, keepdims=True)
    inverse[...] = jnp.broadcast_to(scale, inverse.shape)
    attended = (attended_t[...] * scale).T.astype(jnp.bfloat16)
    attended_ref[...] = attended.reshape(SLABS, 32, WIDTH)
    sums = jnp.sum(attended.astype(jnp.float32).T * cotangent_t[...], axis=0, keepdims=True)
    delta[...] = jnp.broadcast_to(sums, delta.shape)
    grad_query_t[...] = jnp.zeros(grad_query_t.shape, jnp.float32)
    backward_half(query, cotangent, values, keys_t, scores, inverse, delta, grad_query_t, grad_ref, grad_peak)


def third_kernel(
    query, cotangent, values, keys_t, weights, inverse, delta, part_t, grad_query_ref, grad_ref, grad_query_t, grad_peak
):
    grad_query_t[...] = part_t[...]
    backward_half(query, cotangent, values, keys_t, weights, inverse, delta, grad_query_t, grad_ref, grad_peak)
    grad_query = (grad_query_t[...] * SCALE).T.astype(jnp.bfloat16)
    grad_query_ref[...] = grad_query.reshape(SLABS, 32, WIDTH)


def local_call(kernel, name, outs, scratch, passes, has_place):
    def call(*args):
        whole = pl.BlockSpec(memory_space=pltpu.VMEM)
        first = [pl.BlockSpec(memory_space=pltpu.SMEM)] if has_place else []
        return pl.pallas_call(
            kernel,
            out_shape=tuple(jax.ShapeDtypeStruct(shape, dtype) for shape, dtype in outs),
            in_specs=first + [whole] * (len(args) - len(first)),
            out_specs=(whole,) * len(outs),
            scratch_shapes=[pltpu.VMEM(shape, dtype) for shape, dtype in scratch],
            cost_estimate=pl.CostEstimate(
                flops=passes * KEYS * ROWS * WIDTH, bytes_accessed=4 << 20, transcendentals=0
            ),
            compiler_params=pltpu.CompilerParams(vmem_limit_bytes=24 << 20),
            name=name,
        )(*args)

    return call


BF, F32 = jnp.bfloat16, jnp.float32
HALF_ROWS, HALF_COLUMNS = ((KEYS // 2, WIDTH), BF), ((WIDTH, KEYS // 2), BF)
WEIGHTS, STATISTIC, ROWS_T = ((KEYS // 2, ROWS), F32), ((8, ROWS), F32), ((WIDTH, ROWS), F32)
QUERY_ROWS, SENT_ROWS = ((ROWS, WIDTH), BF), ((SLABS, 32, WIDTH), BF)
GRADS, GRAD_PEAK = ((PEERS // 2, 2, SLABS + 1, 8, WIDTH), F32), ((8, WIDTH), F32)

first_part = local_call(
    first_kernel,
    "first_part",
    (QUERY_ROWS, QUERY_ROWS, ROWS_T, HALF_ROWS, HALF_ROWS, HALF_COLUMNS, HALF_COLUMNS, WEIGHTS, STATISTIC),
    (),
    2,
    True,
)
second_part = local_call(
    second_kernel,
    "second_part",
    (SENT_ROWS, GRADS, WEIGHTS, STATISTIC, STATISTIC, ROWS_T),
    (HALF_ROWS, HALF_ROWS, HALF_COLUMNS, HALF_COLUMNS, WEIGHTS, STATISTIC, STATISTIC, ROWS_T, GRAD_PEAK),
    12,
    True,
)
third_part = local_call(third_kernel, "third_part", (SENT_ROWS, GRADS), (ROWS_T, GRAD_PEAK), 7, False)


def fourth(root):
    square = root.astype(jnp.float32) ** 2
    return square * square


def pack_kernel(query_ref, key_ref, value_ref, cotangent_ref, out_ref, narrow, pairs, wide_done, narrow_done):
    small = [
        pltpu.make_async_copy(source, narrow.at[n], narrow_done.at[n])
        for n, source in enumerate((key_ref, value_ref))
    ]
    for copy in small:
        copy.start()
    large = []
    for layer in range(2):
        for token in range(TOKENS):
            for n, source in enumerate((query_ref, cotangent_ref)):
                large.append(
                    pltpu.make_async_copy(
                        source.at[layer, token],
                        out_ref.at[pl.ds(layer * 8, 8), n * TOKENS + token],
                        wide_done.at[n, layer, token],
                    )
                )
    for copy in large:
        copy.start()
    for copy in small:
        copy.wait()
    for layer in range(2):
        for n in range(2):
            pairs[layer, n * TOKENS : (n + 1) * TOKENS] = narrow[n, layer].astype(jnp.float32)
        for group in range(8):
            out_ref[layer * 8 + group, 8] = pairs[layer, :, group, :].astype(jnp.bfloat16)
    for copy in large:
        copy.wait()


def pack(query, key, value, cotangent):
    far = pl.BlockSpec(memory_space=pltpu.HBM)
    by_group = (2, TOKENS, 8, GROUP, WIDTH)
    arrays = (query.reshape(by_group), key, value, cotangent.reshape(by_group))
    packed = pl.pallas_call(
        pack_kernel,
        out_shape=jax.ShapeDtypeStruct((SLABS, 9, 8, WIDTH), jnp.bfloat16),
        in_specs=[far] * 4,
        out_specs=pl.BlockSpec(memory_space=pltpu.VMEM),
        scratch_shapes=[
            pltpu.VMEM((2, 2, TOKENS, 8, WIDTH), jnp.bfloat16),
            pltpu.VMEM((2, 8, 8, WIDTH), jnp.float32),
            pltpu.SemaphoreType.DMA((2, 2, TOKENS)),
            pltpu.SemaphoreType.DMA((2,)),
        ],
        compiler_params=pltpu.CompilerParams(vmem_limit_bytes=4 << 20),
        name="pack",
    )(*[pltpu.with_memory_space_constraint(a, pltpu.HBM) for a in arrays])
    return packed.reshape(SLABS, 72, WIDTH)


def by_token(value, heads):
    value = value.reshape(2, 8, TOKENS, heads, WIDTH).transpose(0, 2, 1, 3, 4)
    return value.reshape(2, TOKENS, 8 * heads, WIDTH)


def on_device(query, key, value, cotangent):
    core = lax.axis_index("c")
    place = jnp.stack([core, lax.axis_index("y") * 4 + lax.axis_index("x")]).astype(jnp.int32)
    rows = lax.all_to_all(pack(query, key, value, cotangent), "z", 0, 0)
    slab = jnp.broadcast_to(rows[:, 64:72, :][None], (PEERS, SLABS, 8, WIDTH))
    mine = lax.all_to_all(slab, PLANE, 0, 0)
    swap = [(0, 1), (1, 0)]
    halves = (PEERS // 2, 2, SLABS, 8, WIDTH)
    other = lax.ppermute(mine, "c", swap)
    query, cotangent, cotangent_t, keys, values, keys_t, values_t, scores, peak = first_part(
        place, rows, mine.reshape(halves)
    )
    attended, other_grad, weights, inverse, delta, part_t = second_part(
        place, other.reshape(halves), query, cotangent, cotangent_t, values_t, scores, peak
    )
    swapped = lax.ppermute(other_grad, "c", swap)
    grad_query, mine_grad = third_part(query, cotangent, values, keys_t, weights, inverse, delta, part_t)
    total = (mine_grad + swapped).reshape(PEERS, SLABS + 1, 8, WIDTH)
    root = jnp.sqrt(jnp.sqrt(jnp.maximum(total[:, SLABS:], 1e-15)))
    root = lax.reduce_precision(root, exponent_bits=5, mantissa_bits=10)
    last = lax.broadcasted_iota(jnp.int32, total.shape, 1) == SLABS
    sent = jnp.where(last, root, total * (FULL / fourth(root))).astype(jnp.float16)
    parts = lax.all_to_all(sent, PLANE, 0, 0)
    scales = fourth(parts[:, SLABS:]) * (1.0 / FULL)
    pair_grad = jnp.sum(parts[:, :SLABS].astype(jnp.float32) * scales, axis=0).astype(jnp.bfloat16)
    back = lax.all_to_all(jnp.concatenate([attended, grad_query, pair_grad], axis=1), "z", 0, 0)
    return (
        by_token(back[:, 0:32], GROUP),
        by_token(back[:, 32:64], GROUP),
        by_token(back[:, 64:68], 1),
        by_token(back[:, 68:72], 1),
    )


def solution(mesh):
    torus = Mesh(mesh.devices.reshape(16, 4, 4, 2), AXES)
    spec = P(None, AXES, None, None)
    return jax.shard_map(
        on_device, mesh=torus, in_specs=(spec,) * 4, out_specs=(spec,) * 4, check_vma=False
    )
```

```python
import functools
import math

import jax
import jax.numpy as jnp
from jax import lax
from jax.experimental import pallas as pl
from jax.experimental.pallas import tpu as pltpu
from jax.sharding import Mesh
from jax.sharding import PartitionSpec as P

AXES = ("z", "y", "x", "c")
PLANE = ("y", "x")
SLABS, PEERS = 16, 16
TOKENS, GROUP, WIDTH = 4, 8, 128
ROWS = SLABS * TOKENS * GROUP
KEYS = 2048
CHUNK = 256
TILE = 128
HIDDEN_SCORE = -1e30
FULL = 2.0**14
SCALE = WIDTH**-0.5
SCALE_LOG2 = SCALE * math.log2(math.e)

NT = (((1,), (1,)), ((), ()))
NN = (((1,), (0,)), ((), ()))


def dot(a, b, dims=NN):
    return lax.dot_general(a, b, dims, preferred_element_type=jnp.float32)


def two_parts(value):
    high = value.astype(jnp.bfloat16)
    return high, (value - high.astype(jnp.float32)).astype(jnp.bfloat16)


def fold_rows(value, op):
    return op(value.reshape(value.shape[0] // 8, 8, value.shape[1]), axis=0)


def sort_half(half_ref, keys, values, keys_t, values_t):
    first = lax.broadcasted_iota(jnp.int32, (PEERS // 2, 8, WIDTH), 1) < 4

    def step(n, carry):
        sorted_keys, sorted_values = [], []
        for slab in range(2):
            even = half_ref[:, 0, 2 * n + slab].astype(jnp.float32)
            odd = half_ref[:, 1, 2 * n + slab].astype(jnp.float32)
            sorted_keys.append(jnp.where(first, even, pltpu.roll(odd, 4, 1)).reshape(64, WIDTH))
            sorted_values.append(jnp.where(first, pltpu.roll(even, 4, 1), odd).reshape(64, WIDTH))
        key, value = jnp.concatenate(sorted_keys, axis=0), jnp.concatenate(sorted_values, axis=0)
        at = pl.ds(pl.multiple_of(n * TILE, TILE), TILE)
        keys[at, :] = key.astype(jnp.bfloat16)
        values[at, :] = value.astype(jnp.bfloat16)
        keys_t[:, at] = key.T.astype(jnp.bfloat16)
        values_t[:, at] = value.T.astype(jnp.bfloat16)
        return carry

    lax.fori_loop(0, SLABS // 2, step, 0, unroll=4)


def chunks():
    for b in range(ROWS // TILE):
        yield b * TILE, slice(b * CHUNK, (b + 1) * CHUNK)


def score_half(keys, query, scores, peak, core, place, key_core):
    for low, at in chunks():
        s = dot(keys[at, :], query[low:, :], NT) * SCALE_LOG2
        key = at.start + lax.broadcasted_iota(jnp.int32, (CHUNK, TILE), 0)
        key_at = (key // 64) * 128 + ((key % 64) // 4) * 8 + key_core * 4 + key % 4
        row = low + lax.broadcasted_iota(jnp.int32, (CHUNK, TILE), 1)
        row_at = (row // 32) * 128 + place * 8 + core * 4 + (row % 32) // 8
        near = jnp.where(key_at <= row_at, s[:, :TILE], HIDDEN_SCORE)
        scores[at, low : low + TILE] = near
        peak[:, low : low + TILE] = jnp.maximum(peak[:, low : low + TILE], fold_rows(near, jnp.max))
        if low + TILE < ROWS:
            far = s[:, TILE:]
            scores[at, low + TILE :] = far
            peak[:, low + TILE :] = jnp.maximum(peak[:, low + TILE :], fold_rows(far, jnp.max))


def forward_half(scores, weights, values_t, peak, total, attended_t):
    for low, at in chunks():
        p = jnp.exp2(scores[at, low:] - peak[0:1, low:])
        weights[at, low:] = p
        total[:, low:] += fold_rows(p, jnp.sum)
        high, rest = two_parts(p)
        v = values_t[:, at]
        attended_t[:, low:] += dot(v, high) + dot(v, rest)


def add_query_grad(low, at, keys_t, d_high, d_rest, grad_query_t):
    k = keys_t[:, at]
    grad_query_t[:, low:] += dot(k, d_high) + dot(k, d_rest)


def backward_half(query, cotangent, values, weights, inverse, delta, grad_ref, grad_peak, take_dscore):
    first = lax.broadcasted_iota(jnp.int32, (PEERS // 2, 8, WIDTH), 1) < 4
    grad_peak[...] = jnp.zeros(grad_peak.shape, jnp.float32)
    for low, at in chunks():
        grad = dot(values[at, :], cotangent[low:, :], NT)
        p = weights[at, low:] * inverse[0:1, low:]
        p_high, p_rest = two_parts(p)
        d_high, d_rest = two_parts(p * (grad - delta[0:1, low:]))
        value_grad = dot(p_high, cotangent[low:, :]) + dot(p_rest, cotangent[low:, :])
        key_grad = SCALE * (dot(d_high, query[low:, :]) + dot(d_rest, query[low:, :]))
        take_dscore(low, at, d_high, d_rest)
        both = jnp.maximum(jnp.abs(key_grad), jnp.abs(value_grad))
        grad_peak[...] = jnp.maximum(grad_peak[...], fold_rows(both, jnp.max))
        for n in range(CHUNK // 64):
            kg = key_grad[n * 64 : (n + 1) * 64].reshape(PEERS // 2, 8, WIDTH)
            vg = value_grad[n * 64 : (n + 1) * 64].reshape(PEERS // 2, 8, WIDTH)
            slab = at.start // 64 + n
            grad_ref[:, 0, slab] = jnp.where(first, kg, pltpu.roll(vg, 4, 1))
            grad_ref[:, 1, slab] = jnp.where(first, pltpu.roll(kg, 4, 1), vg)
    grad_ref[:, :, SLABS] = jnp.full((PEERS // 2, 2, 8, WIDTH), jnp.max(grad_peak[...]), jnp.float32)


def first_kernel(
    place_ref, rows_ref, mine_ref, query, cotangent, cotangent_t, keys, values, keys_t, values_t, scores, peak
):
    query[...] = rows_ref[:, 0:32, :].reshape(ROWS, WIDTH)
    cotangent[...] = rows_ref[:, 32:64, :].reshape(ROWS, WIDTH)
    sort_half(mine_ref, keys, values, keys_t, values_t)
    cotangent_t[...] = cotangent[...].astype(jnp.float32).T
    peak[...] = jnp.full(peak.shape, HIDDEN_SCORE, jnp.float32)
    score_half(keys, query, scores, peak, place_ref[0], place_ref[1], place_ref[0])


def second_kernel(
    place_ref,
    other_ref,
    query,
    cotangent,
    cotangent_t,
    mine_values_t,
    mine_scores,
    mine_peak,
    grad_ref,
    mine_weights,
    inverse,
    delta,
    rounded_t,
    keys_t,
    dscore_high,
    dscore_rest,
    keys,
    values,
    values_t,
    scores,
    peak,
    total,
    attended_t,
    grad_peak,
):
    sort_half(other_ref, keys, values, keys_t, values_t)
    peak[...] = mine_peak[...]
    score_half(keys, query, scores, peak, place_ref[0], place_ref[1], 1 - place_ref[0])
    peak[...] = jnp.broadcast_to(jnp.max(peak[...], axis=0, keepdims=True), peak.shape)
    total[...] = jnp.zeros(total.shape, jnp.float32)
    attended_t[...] = jnp.zeros(attended_t.shape, jnp.float32)
    forward_half(mine_scores, mine_weights, mine_values_t, peak, total, attended_t)
    forward_half(scores, scores, values_t, peak, total, attended_t)
    scale = 1.0 / jnp.sum(total[...], axis=0, keepdims=True)
    inverse[...] = jnp.broadcast_to(scale, inverse.shape)
    attended = (attended_t[...] * scale).astype(jnp.bfloat16).astype(jnp.float32)
    rounded_t[...] = attended
    delta[...] = jnp.broadcast_to(jnp.sum(attended * cotangent_t[...], axis=0, keepdims=True), delta.shape)

    def keep(low, at, d_high, d_rest):
        dscore_high[at, low:] = d_high
        dscore_rest[at, low:] = d_rest

    backward_half(query, cotangent, values, scores, inverse, delta, grad_ref, grad_peak, keep)


def third_kernel(
    query,
    cotangent,
    values,
    keys_t,
    weights,
    inverse,
    delta,
    rounded_t,
    other_keys_t,
    dscore_high,
    dscore_rest,
    out_ref,
    grad_ref,
    grad_query_t,
    grad_peak,
):
    attended = rounded_t[...].T.astype(jnp.bfloat16)
    out_ref[:, 0:32, :] = attended.reshape(SLABS, 32, WIDTH)
    grad_query_t[...] = jnp.zeros(grad_query_t.shape, jnp.float32)

    def add(low, at, d_high, d_rest):
        add_query_grad(low, at, keys_t, d_high, d_rest, grad_query_t)

    backward_half(query, cotangent, values, weights, inverse, delta, grad_ref, grad_peak, add)
    for low, at in chunks():
        add_query_grad(low, at, other_keys_t, dscore_high[at, low:], dscore_rest[at, low:], grad_query_t)
    grad_query = (grad_query_t[...] * SCALE).T.astype(jnp.bfloat16)
    out_ref[:, 32:64, :] = grad_query.reshape(SLABS, 32, WIDTH)


def local_call(kernel, name, outs, scratch, passes, has_place):
    def call(*args):
        whole = pl.BlockSpec(memory_space=pltpu.VMEM)
        first = [pl.BlockSpec(memory_space=pltpu.SMEM)] if has_place else []
        return pl.pallas_call(
            kernel,
            out_shape=tuple(jax.ShapeDtypeStruct(shape, dtype) for shape, dtype in outs),
            in_specs=first + [whole] * (len(args) - len(first)),
            out_specs=(whole,) * len(outs),
            scratch_shapes=[pltpu.VMEM(shape, dtype) for shape, dtype in scratch],
            cost_estimate=pl.CostEstimate(
                flops=passes * KEYS * ROWS * WIDTH, bytes_accessed=4 << 20, transcendentals=0
            ),
            compiler_params=pltpu.CompilerParams(vmem_limit_bytes=24 << 20),
            name=name,
        )(*args)

    return call


BF, F32 = jnp.bfloat16, jnp.float32
HALF_ROWS, HALF_COLUMNS = ((KEYS // 2, WIDTH), BF), ((WIDTH, KEYS // 2), BF)
WEIGHTS, STATISTIC, ROWS_T = ((KEYS // 2, ROWS), F32), ((8, ROWS), F32), ((WIDTH, ROWS), F32)
QUERY_ROWS, SENT_ROWS = ((ROWS, WIDTH), BF), ((SLABS, 64, WIDTH), BF)
DSCORES = ((KEYS // 2, ROWS), BF)
GRADS, GRAD_PEAK = ((PEERS // 2, 2, SLABS + 1, 8, WIDTH), F32), ((8, WIDTH), F32)

first_part = local_call(
    first_kernel,
    "first_part",
    (QUERY_ROWS, QUERY_ROWS, ROWS_T, HALF_ROWS, HALF_ROWS, HALF_COLUMNS, HALF_COLUMNS, WEIGHTS, STATISTIC),
    (),
    2,
    True,
)
second_part = local_call(
    second_kernel,
    "second_part",
    (GRADS, WEIGHTS, STATISTIC, STATISTIC, ROWS_T, HALF_COLUMNS, DSCORES, DSCORES),
    (HALF_ROWS, HALF_ROWS, HALF_COLUMNS, WEIGHTS, STATISTIC, STATISTIC, ROWS_T, GRAD_PEAK),
    10,
    True,
)
third_part = local_call(third_kernel, "third_part", (SENT_ROWS, GRADS), (ROWS_T, GRAD_PEAK), 9, False)


def fourth(root):
    square = root.astype(jnp.float32) ** 2
    return square * square


def pack_kernel(query_ref, key_ref, value_ref, cotangent_ref, out_ref, narrow, pairs, wide_done, narrow_done):
    small = [
        pltpu.make_async_copy(source, narrow.at[n], narrow_done.at[n])
        for n, source in enumerate((key_ref, value_ref))
    ]
    for copy in small:
        copy.start()
    large = []
    for layer in range(2):
        for token in range(TOKENS):
            for n, source in enumerate((query_ref, cotangent_ref)):
                large.append(
                    pltpu.make_async_copy(
                        source.at[layer, token],
                        out_ref.at[pl.ds(layer * 8, 8), n * TOKENS + token],
                        wide_done.at[n, layer, token],
                    )
                )
    for copy in large:
        copy.start()
    for copy in small:
        copy.wait()
    for layer in range(2):
        for n in range(2):
            pairs[layer, n * TOKENS : (n + 1) * TOKENS] = narrow[n, layer].astype(jnp.float32)
        for group in range(8):
            out_ref[layer * 8 + group, 8] = pairs[layer, :, group, :].astype(jnp.bfloat16)
    for copy in large:
        copy.wait()


def pack(query, key, value, cotangent):
    far = pl.BlockSpec(memory_space=pltpu.HBM)
    by_group = (2, TOKENS, 8, GROUP, WIDTH)
    arrays = (query.reshape(by_group), key, value, cotangent.reshape(by_group))
    packed = pl.pallas_call(
        pack_kernel,
        out_shape=jax.ShapeDtypeStruct((SLABS, 9, 8, WIDTH), jnp.bfloat16),
        in_specs=[far] * 4,
        out_specs=pl.BlockSpec(memory_space=pltpu.VMEM),
        scratch_shapes=[
            pltpu.VMEM((2, 2, TOKENS, 8, WIDTH), jnp.bfloat16),
            pltpu.VMEM((2, 8, 8, WIDTH), jnp.float32),
            pltpu.SemaphoreType.DMA((2, 2, TOKENS)),
            pltpu.SemaphoreType.DMA((2,)),
        ],
        compiler_params=pltpu.CompilerParams(vmem_limit_bytes=4 << 20),
        name="pack",
    )(*[pltpu.with_memory_space_constraint(a, pltpu.HBM) for a in arrays])
    return packed.reshape(SLABS, 72, WIDTH)


def unpack_kernel(
    back_ref, attended_ref, grad_query_ref, grad_key_ref, grad_value_ref, narrow, pairs, wide_done, narrow_done
):
    copies = []
    for layer in range(2):
        for token in range(TOKENS):
            for n, target in enumerate((attended_ref, grad_query_ref)):
                copies.append(
                    pltpu.make_async_copy(
                        back_ref.at[pl.ds(layer * 8, 8), n * TOKENS + token],
                        target.at[layer, token],
                        wide_done.at[n, layer, token],
                    )
                )
    for copy in copies:
        copy.start()
    for layer in range(2):
        for group in range(8):
            pairs[layer, :, group, :] = back_ref[layer * 8 + group, 8].astype(jnp.float32)
        for n in range(2):
            narrow[n, layer] = pairs[layer, n * TOKENS : (n + 1) * TOKENS].astype(jnp.bfloat16)
    small = [
        pltpu.make_async_copy(narrow.at[n], target, narrow_done.at[n])
        for n, target in enumerate((grad_key_ref, grad_value_ref))
    ]
    for copy in small:
        copy.start()
    for copy in copies + small:
        copy.wait()


def unpack(back):
    far = pl.BlockSpec(memory_space=pltpu.HBM)
    wide = jax.ShapeDtypeStruct((2, TOKENS, 8, GROUP, WIDTH), jnp.bfloat16)
    thin = jax.ShapeDtypeStruct((2, TOKENS, 8, WIDTH), jnp.bfloat16)
    attended, grad_query, grad_key, grad_value = pl.pallas_call(
        unpack_kernel,
        out_shape=(wide, wide, thin, thin),
        in_specs=[pl.BlockSpec(memory_space=pltpu.VMEM)],
        out_specs=(far,) * 4,
        scratch_shapes=[
            pltpu.VMEM((2, 2, TOKENS, 8, WIDTH), jnp.bfloat16),
            pltpu.VMEM((2, 8, 8, WIDTH), jnp.float32),
            pltpu.SemaphoreType.DMA((2, 2, TOKENS)),
            pltpu.SemaphoreType.DMA((2,)),
        ],
        compiler_params=pltpu.CompilerParams(vmem_limit_bytes=4 << 20),
        name="unpack",
    )(back.reshape(SLABS, 9, 8, WIDTH))
    heads = (2, TOKENS, 64, WIDTH)
    return attended.reshape(heads), grad_query.reshape(heads), grad_key, grad_value


def on_device(query, key, value, cotangent):
    core = lax.axis_index("c")
    place = jnp.stack([core, lax.axis_index("y") * 4 + lax.axis_index("x")]).astype(jnp.int32)
    rows = lax.all_to_all(pack(query, key, value, cotangent), "z", 0, 0)
    slab = jnp.broadcast_to(rows[:, 64:72, :][None], (PEERS, SLABS, 8, WIDTH))
    mine = lax.all_to_all(slab, PLANE, 0, 0)
    swap = [(0, 1), (1, 0)]
    halves = (PEERS // 2, 2, SLABS, 8, WIDTH)
    other = lax.ppermute(mine, "c", swap)
    query, cotangent, cotangent_t, keys, values, keys_t, values_t, scores, peak = first_part(
        place, rows, mine.reshape(halves)
    )
    other_grad, weights, inverse, delta, *rest = second_part(
        place, other.reshape(halves), query, cotangent, cotangent_t, values_t, scores, peak
    )
    swapped = lax.ppermute(other_grad, "c", swap)
    out, mine_grad = third_part(query, cotangent, values, keys_t, weights, inverse, delta, *rest)
    total = (mine_grad + swapped).reshape(PEERS, SLABS + 1, 8, WIDTH)
    root = jnp.sqrt(jnp.sqrt(jnp.maximum(total[:, SLABS:], 1e-15)))
    root = lax.reduce_precision(root, exponent_bits=5, mantissa_bits=10)
    last = lax.broadcasted_iota(jnp.int32, total.shape, 1) == SLABS
    sent = jnp.where(last, root, total * (FULL / fourth(root))).astype(jnp.float16)
    parts = lax.all_to_all(sent, PLANE, 0, 0)
    scales = fourth(parts[:, SLABS:]) * (1.0 / FULL)
    pair_grad = jnp.sum(parts[:, :SLABS].astype(jnp.float32) * scales, axis=0).astype(jnp.bfloat16)
    back = lax.all_to_all(jnp.concatenate([out, pair_grad], axis=1), "z", 0, 0)
    return unpack(back)


def solution(mesh):
    torus = Mesh(mesh.devices.reshape(16, 4, 4, 2), AXES)
    spec = P(None, AXES, None, None)
    return jax.shard_map(
        on_device, mesh=torus, in_specs=(spec,) * 4, out_specs=(spec,) * 4, check_vma=False
    )
```

```python
import math

import jax
import jax.numpy as jnp
from jax import lax
from jax.experimental import pallas as pl
from jax.experimental.pallas import tpu as pltpu
from jax.sharding import Mesh
from jax.sharding import PartitionSpec as P


AXES = ("z", "y", "x", "c")
PLANE = ("y", "x")
SLABS, PEERS = 16, 16
TOKENS, GROUP, WIDTH = 4, 8, 128
ROWS = SLABS * TOKENS * GROUP
KEYS = 2048
CHUNK = 256
TILE = 128
HIDDEN_SCORE = -1e30
FULL = 2.0**14
SCALE = WIDTH**-0.5
SCALE_LOG2 = SCALE * math.log2(math.e)

NT = (((1,), (1,)), ((), ()))
NN = (((1,), (0,)), ((), ()))


def dot(a, b, dims=NN):
    return lax.dot_general(a, b, dims, preferred_element_type=jnp.float32)


def two_parts(value):
    high = value.astype(jnp.bfloat16)
    return high, (value - high.astype(jnp.float32)).astype(jnp.bfloat16)


def fold_rows(value, op):
    return op(value.reshape(value.shape[0] // 8, 8, value.shape[1]), axis=0)


def sort_half(half_ref, keys, values, keys_t, values_t):
    first = lax.broadcasted_iota(jnp.int32, (PEERS // 2, 8, WIDTH), 1) < 4

    def step(n, carry):
        sorted_keys, sorted_values = [], []
        for slab in range(2):
            even = half_ref[:, 0, 2 * n + slab].astype(jnp.float32)
            odd = half_ref[:, 1, 2 * n + slab].astype(jnp.float32)
            sorted_keys.append(jnp.where(first, even, pltpu.roll(odd, 4, 1)).reshape(64, WIDTH))
            sorted_values.append(jnp.where(first, pltpu.roll(even, 4, 1), odd).reshape(64, WIDTH))
        key, value = jnp.concatenate(sorted_keys, axis=0), jnp.concatenate(sorted_values, axis=0)
        at = pl.ds(pl.multiple_of(n * TILE, TILE), TILE)
        keys[at, :] = key.astype(jnp.bfloat16)
        values[at, :] = value.astype(jnp.bfloat16)
        keys_t[:, at] = key.T.astype(jnp.bfloat16)
        values_t[:, at] = value.T.astype(jnp.bfloat16)
        return carry

    lax.fori_loop(0, SLABS // 2, step, 0, unroll=4)


def chunks():
    for b in range(ROWS // TILE):
        yield b * TILE, slice(b * CHUNK, (b + 1) * CHUNK)


def score_half(keys, query, scores, peak, core, place, key_core):
    for low, at in chunks():
        s = dot(keys[at, :], query[low:, :], NT) * SCALE_LOG2
        key = at.start + lax.broadcasted_iota(jnp.int32, (CHUNK, TILE), 0)
        key_at = (key // 64) * 128 + ((key % 64) // 4) * 8 + key_core * 4 + key % 4
        row = low + lax.broadcasted_iota(jnp.int32, (CHUNK, TILE), 1)
        row_at = (row // 32) * 128 + place * 8 + core * 4 + (row % 32) // 8
        near = jnp.where(key_at <= row_at, s[:, :TILE], HIDDEN_SCORE)
        scores[at, low : low + TILE] = near
        peak[:, low : low + TILE] = jnp.maximum(peak[:, low : low + TILE], fold_rows(near, jnp.max))
        if low + TILE < ROWS:
            far = s[:, TILE:]
            scores[at, low + TILE :] = far
            peak[:, low + TILE :] = jnp.maximum(peak[:, low + TILE :], fold_rows(far, jnp.max))


def forward_half(scores, weights, values_t, peak, total, attended_t):
    for low, at in chunks():
        p = jnp.exp2(scores[at, low:] - peak[0:1, low:])
        weights[at, low:] = p
        total[:, low:] += fold_rows(p, jnp.sum)
        high, rest = two_parts(p)
        v = values_t[:, at]
        attended_t[:, low:] += dot(v, high) + dot(v, rest)


def add_query_grad(low, at, keys_t, d_high, d_rest, grad_query_t):
    k = keys_t[:, at]
    grad_query_t[:, low:] += dot(k, d_high) + dot(k, d_rest)


def backward_half(query, cotangent, values, weights, inverse, delta, grad_ref, grad_peak, take_dscore):
    first = lax.broadcasted_iota(jnp.int32, (PEERS // 2, 8, WIDTH), 1) < 4
    grad_peak[...] = jnp.zeros(grad_peak.shape, jnp.float32)
    for low, at in chunks():
        grad = dot(values[at, :], cotangent[low:, :], NT)
        p = weights[at, low:] * inverse[0:1, low:]
        p_high, p_rest = two_parts(p)
        d_high, d_rest = two_parts(p * (grad - delta[0:1, low:]))
        value_grad = dot(p_high, cotangent[low:, :]) + dot(p_rest, cotangent[low:, :])
        key_grad = SCALE * (dot(d_high, query[low:, :]) + dot(d_rest, query[low:, :]))
        take_dscore(low, at, d_high, d_rest)
        both = jnp.maximum(jnp.abs(key_grad), jnp.abs(value_grad))
        grad_peak[...] = jnp.maximum(grad_peak[...], fold_rows(both, jnp.max))
        for n in range(CHUNK // 64):
            kg = key_grad[n * 64 : (n + 1) * 64].reshape(PEERS // 2, 8, WIDTH)
            vg = value_grad[n * 64 : (n + 1) * 64].reshape(PEERS // 2, 8, WIDTH)
            slab = at.start // 64 + n
            grad_ref[:, 0, slab] = jnp.where(first, kg, pltpu.roll(vg, 4, 1))
            grad_ref[:, 1, slab] = jnp.where(first, pltpu.roll(kg, 4, 1), vg)
    grad_ref[:, :, SLABS] = jnp.full((PEERS // 2, 2, 8, WIDTH), jnp.max(grad_peak[...]), jnp.float32)


def prepare_kernel(rows_ref, query, cotangent, cotangent_t):
    query[...] = rows_ref[:, 0:32, :].reshape(ROWS, WIDTH)
    cotangent[...] = rows_ref[:, 32:64, :].reshape(ROWS, WIDTH)
    cotangent_t[...] = cotangent[...].astype(jnp.float32).T


def first_kernel(
    place_ref, mine_ref, query, keys_t, values, weights, peak, total, attended_t, keys, values_t
):
    sort_half(mine_ref, keys, values, keys_t, values_t)
    peak[...] = jnp.full(peak.shape, HIDDEN_SCORE, jnp.float32)
    score_half(keys, query, weights, peak, place_ref[0], place_ref[1], place_ref[0])
    peak[...] = jnp.broadcast_to(jnp.max(peak[...], axis=0, keepdims=True), peak.shape)
    total[...] = jnp.zeros(total.shape, jnp.float32)
    attended_t[...] = jnp.zeros(attended_t.shape, jnp.float32)
    forward_half(weights, weights, values_t, peak, total, attended_t)


def second_kernel(
    place_ref,
    other_ref,
    query,
    cotangent,
    cotangent_t,
    mine_peak,
    mine_total,
    mine_attended_t,
    grad_ref,
    mine_inverse,
    delta,
    rounded_t,
    keys_t,
    dscore_high,
    dscore_rest,
    keys,
    values,
    values_t,
    scores,
    peak,
    total,
    inverse,
    attended_t,
    grad_peak,
):
    sort_half(other_ref, keys, values, keys_t, values_t)
    peak[...] = mine_peak[...]
    score_half(keys, query, scores, peak, place_ref[0], place_ref[1], 1 - place_ref[0])
    peak[...] = jnp.broadcast_to(jnp.max(peak[...], axis=0, keepdims=True), peak.shape)
    shrink = jnp.exp2(mine_peak[0:1, :] - peak[0:1, :])
    total[...] = mine_total[...] * shrink
    attended_t[...] = mine_attended_t[...] * shrink
    forward_half(scores, scores, values_t, peak, total, attended_t)
    scale = 1.0 / jnp.sum(total[...], axis=0, keepdims=True)
    inverse[...] = jnp.broadcast_to(scale, inverse.shape)
    mine_inverse[...] = jnp.broadcast_to(scale * shrink, mine_inverse.shape)
    attended = (attended_t[...] * scale).astype(jnp.bfloat16).astype(jnp.float32)
    rounded_t[...] = attended
    delta[...] = jnp.broadcast_to(jnp.sum(attended * cotangent_t[...], axis=0, keepdims=True), delta.shape)

    def keep(low, at, d_high, d_rest):
        dscore_high[at, low:] = d_high
        dscore_rest[at, low:] = d_rest

    backward_half(query, cotangent, values, scores, inverse, delta, grad_ref, grad_peak, keep)


def third_kernel(
    query,
    cotangent,
    values,
    keys_t,
    weights,
    inverse,
    delta,
    rounded_t,
    other_keys_t,
    dscore_high,
    dscore_rest,
    out_ref,
    grad_ref,
    grad_query_t,
    grad_peak,
):
    attended = rounded_t[...].T.astype(jnp.bfloat16)
    out_ref[:, 0:32, :] = attended.reshape(SLABS, 32, WIDTH)
    grad_query_t[...] = jnp.zeros(grad_query_t.shape, jnp.float32)

    def add(low, at, d_high, d_rest):
        add_query_grad(low, at, keys_t, d_high, d_rest, grad_query_t)

    backward_half(query, cotangent, values, weights, inverse, delta, grad_ref, grad_peak, add)
    for low, at in chunks():
        add_query_grad(low, at, other_keys_t, dscore_high[at, low:], dscore_rest[at, low:], grad_query_t)
    grad_query = (grad_query_t[...] * SCALE).T.astype(jnp.bfloat16)
    out_ref[:, 32:64, :] = grad_query.reshape(SLABS, 32, WIDTH)


def local_call(kernel, outs, scratch, passes, has_place):
    def call(*args):
        whole = pl.BlockSpec(memory_space=pltpu.VMEM)
        first = [pl.BlockSpec(memory_space=pltpu.SMEM)] if has_place else []
        return pl.pallas_call(
            kernel,
            out_shape=tuple(jax.ShapeDtypeStruct(shape, dtype) for shape, dtype in outs),
            in_specs=first + [whole] * (len(args) - len(first)),
            out_specs=(whole,) * len(outs),
            scratch_shapes=[pltpu.VMEM(shape, dtype) for shape, dtype in scratch],
            cost_estimate=pl.CostEstimate(
                flops=passes * KEYS * ROWS * WIDTH, bytes_accessed=4 << 20, transcendentals=0
            ),
            compiler_params=pltpu.CompilerParams(vmem_limit_bytes=24 << 20),
        )(*args)

    return call


BF, F32 = jnp.bfloat16, jnp.float32
HALF_ROWS, HALF_COLUMNS = ((KEYS // 2, WIDTH), BF), ((WIDTH, KEYS // 2), BF)
WEIGHTS, STATISTIC, ROWS_T = ((KEYS // 2, ROWS), F32), ((8, ROWS), F32), ((WIDTH, ROWS), F32)
QUERY_ROWS, SENT_ROWS = ((ROWS, WIDTH), BF), ((SLABS, 64, WIDTH), BF)
DSCORES = ((KEYS // 2, ROWS), BF)
GRADS, GRAD_PEAK = ((PEERS // 2, 2, SLABS + 1, 8, WIDTH), F32), ((8, WIDTH), F32)

prepare = local_call(prepare_kernel, (QUERY_ROWS, QUERY_ROWS, ROWS_T), (), 1, False)
first_part = local_call(
    first_kernel, (HALF_COLUMNS, HALF_ROWS, WEIGHTS, STATISTIC, STATISTIC, ROWS_T), (HALF_ROWS, HALF_COLUMNS), 4, True
)
second_part = local_call(
    second_kernel,
    (GRADS, STATISTIC, STATISTIC, ROWS_T, HALF_COLUMNS, DSCORES, DSCORES),
    (HALF_ROWS, HALF_ROWS, HALF_COLUMNS, WEIGHTS, STATISTIC, STATISTIC, STATISTIC, ROWS_T, GRAD_PEAK),
    8,
    True,
)
third_part = local_call(third_kernel, (SENT_ROWS, GRADS), (ROWS_T, GRAD_PEAK), 9, False)


def fourth(root):
    square = root.astype(jnp.float32) ** 2
    return square * square


def pack_kernel(query_ref, key_ref, value_ref, cotangent_ref, out_ref, narrow, pairs, wide_done, narrow_done):
    small = [
        pltpu.make_async_copy(source, narrow.at[n], narrow_done.at[n])
        for n, source in enumerate((key_ref, value_ref))
    ]
    for copy in small:
        copy.start()
    large = []
    for layer in range(2):
        for token in range(TOKENS):
            for n, source in enumerate((query_ref, cotangent_ref)):
                large.append(
                    pltpu.make_async_copy(
                        source.at[layer, token],
                        out_ref.at[pl.ds(layer * 8, 8), n * TOKENS + token],
                        wide_done.at[n, layer, token],
                    )
                )
    for copy in large:
        copy.start()
    for copy in small:
        copy.wait()
    for layer in range(2):
        for n in range(2):
            pairs[layer, n * TOKENS : (n + 1) * TOKENS] = narrow[n, layer].astype(jnp.float32)
        for group in range(8):
            out_ref[layer * 8 + group, 8] = pairs[layer, :, group, :].astype(jnp.bfloat16)
    for copy in large:
        copy.wait()


def pack(query, key, value, cotangent):
    far = pl.BlockSpec(memory_space=pltpu.HBM)
    by_group = (2, TOKENS, 8, GROUP, WIDTH)
    arrays = (query.reshape(by_group), key, value, cotangent.reshape(by_group))
    packed = pl.pallas_call(
        pack_kernel,
        out_shape=jax.ShapeDtypeStruct((SLABS, 9, 8, WIDTH), jnp.bfloat16),
        in_specs=[far] * 4,
        out_specs=pl.BlockSpec(memory_space=pltpu.VMEM),
        scratch_shapes=[
            pltpu.VMEM((2, 2, TOKENS, 8, WIDTH), jnp.bfloat16),
            pltpu.VMEM((2, 8, 8, WIDTH), jnp.float32),
            pltpu.SemaphoreType.DMA((2, 2, TOKENS)),
            pltpu.SemaphoreType.DMA((2,)),
        ],
        compiler_params=pltpu.CompilerParams(vmem_limit_bytes=4 << 20),
        name="pack",
    )(*[pltpu.with_memory_space_constraint(a, pltpu.HBM) for a in arrays])
    return packed.reshape(SLABS, 72, WIDTH)


def unpack_kernel(
    back_ref, attended_ref, grad_query_ref, grad_key_ref, grad_value_ref, narrow, pairs, wide_done, narrow_done
):
    copies = []
    for layer in range(2):
        for token in range(TOKENS):
            for n, target in enumerate((attended_ref, grad_query_ref)):
                copies.append(
                    pltpu.make_async_copy(
                        back_ref.at[pl.ds(layer * 8, 8), n * TOKENS + token],
                        target.at[layer, token],
                        wide_done.at[n, layer, token],
                    )
                )
    for copy in copies:
        copy.start()
    for layer in range(2):
        for group in range(8):
            pairs[layer, :, group, :] = back_ref[layer * 8 + group, 8].astype(jnp.float32)
        for n in range(2):
            narrow[n, layer] = pairs[layer, n * TOKENS : (n + 1) * TOKENS].astype(jnp.bfloat16)
    small = [
        pltpu.make_async_copy(narrow.at[n], target, narrow_done.at[n])
        for n, target in enumerate((grad_key_ref, grad_value_ref))
    ]
    for copy in small:
        copy.start()
    for copy in copies + small:
        copy.wait()


def unpack(back):
    far = pl.BlockSpec(memory_space=pltpu.HBM)
    wide = jax.ShapeDtypeStruct((2, TOKENS, 8, GROUP, WIDTH), jnp.bfloat16)
    thin = jax.ShapeDtypeStruct((2, TOKENS, 8, WIDTH), jnp.bfloat16)
    attended, grad_query, grad_key, grad_value = pl.pallas_call(
        unpack_kernel,
        out_shape=(wide, wide, thin, thin),
        in_specs=[pl.BlockSpec(memory_space=pltpu.VMEM)],
        out_specs=(far,) * 4,
        scratch_shapes=[
            pltpu.VMEM((2, 2, TOKENS, 8, WIDTH), jnp.bfloat16),
            pltpu.VMEM((2, 8, 8, WIDTH), jnp.float32),
            pltpu.SemaphoreType.DMA((2, 2, TOKENS)),
            pltpu.SemaphoreType.DMA((2,)),
        ],
        compiler_params=pltpu.CompilerParams(vmem_limit_bytes=4 << 20),
        name="unpack",
    )(back.reshape(SLABS, 9, 8, WIDTH))
    heads = (2, TOKENS, 64, WIDTH)
    return attended.reshape(heads), grad_query.reshape(heads), grad_key, grad_value


def on_device(query, key, value, cotangent):
    core = lax.axis_index("c")
    place = jnp.stack([core, lax.axis_index("y") * 4 + lax.axis_index("x")]).astype(jnp.int32)
    rows = lax.all_to_all(pack(query, key, value, cotangent), "z", 0, 0)
    slab = jnp.broadcast_to(rows[:, 64:72, :][None], (PEERS, SLABS, 8, WIDTH))
    mine = lax.all_to_all(slab, PLANE, 0, 0)
    query, cotangent, cotangent_t = prepare(rows)
    swap = [(0, 1), (1, 0)]
    halves = (PEERS // 2, 2, SLABS, 8, WIDTH)
    other = lax.ppermute(mine, "c", swap)
    keys_t, values, weights, *forward = first_part(place, mine.reshape(halves), query)
    other_grad, inverse, delta, *rest = second_part(
        place, other.reshape(halves), query, cotangent, cotangent_t, *forward
    )
    swapped = lax.ppermute(other_grad, "c", swap)
    out, mine_grad = third_part(query, cotangent, values, keys_t, weights, inverse, delta, *rest)
    total = (mine_grad + swapped).reshape(PEERS, SLABS + 1, 8, WIDTH)
    root = jnp.sqrt(jnp.sqrt(jnp.maximum(total[:, SLABS:], 1e-15)))
    root = lax.reduce_precision(root, exponent_bits=5, mantissa_bits=10)
    last = lax.broadcasted_iota(jnp.int32, total.shape, 1) == SLABS
    sent = jnp.where(last, root, total * (FULL / fourth(root))).astype(jnp.float16)
    parts = lax.all_to_all(sent, PLANE, 0, 0)
    scales = fourth(parts[:, SLABS:]) * (1.0 / FULL)
    pair_grad = jnp.sum(parts[:, :SLABS].astype(jnp.float32) * scales, axis=0).astype(jnp.bfloat16)
    back = lax.all_to_all(jnp.concatenate([out, pair_grad], axis=1), "z", 0, 0)
    return unpack(back)


def solution(mesh):
    torus = Mesh(mesh.devices.reshape(16, 4, 4, 2), AXES)
    spec = P(None, AXES, None, None)
    return jax.shard_map(
        on_device, mesh=torus, in_specs=(spec,) * 4, out_specs=(spec,) * 4, check_vma=False
    )
```

```python
import functools
import math

import jax
import jax.numpy as jnp
from jax import lax
from jax.experimental import pallas as pl
from jax.experimental.pallas import tpu as pltpu
from jax.sharding import Mesh
from jax.sharding import PartitionSpec as P

AXES = ("z", "y", "x", "c")
PLANE = ("y", "x")
SLABS, PEERS = 16, 16
TOKENS, GROUP, WIDTH = 4, 8, 128
ROWS = SLABS * TOKENS * GROUP
KEYS = 2048
CHUNK = 256
TILE = 128
HIDDEN_SCORE = -1e30
FULL = 2.0**14
SCALE = WIDTH**-0.5
SCALE_LOG2 = SCALE * math.log2(math.e)

NT = (((1,), (1,)), ((), ()))
NN = (((1,), (0,)), ((), ()))


def dot(a, b, dims=NN):
    return lax.dot_general(a, b, dims, preferred_element_type=jnp.float32)


def two_parts(value):
    high = value.astype(jnp.bfloat16)
    return high, (value - high.astype(jnp.float32)).astype(jnp.bfloat16)


def fold_rows(value, op):
    return op(value.reshape(value.shape[0] // 8, 8, value.shape[1]), axis=0)


def sort_half(half_ref, keys, values, keys_t, values_t):
    first = lax.broadcasted_iota(jnp.int32, (PEERS // 2, 8, WIDTH), 1) < 4

    def step(n, carry):
        sorted_keys, sorted_values = [], []
        for slab in range(2):
            even = half_ref[:, 0, 2 * n + slab].astype(jnp.float32)
            odd = half_ref[:, 1, 2 * n + slab].astype(jnp.float32)
            sorted_keys.append(jnp.where(first, even, pltpu.roll(odd, 4, 1)).reshape(64, WIDTH))
            sorted_values.append(jnp.where(first, pltpu.roll(even, 4, 1), odd).reshape(64, WIDTH))
        key, value = jnp.concatenate(sorted_keys, axis=0), jnp.concatenate(sorted_values, axis=0)
        at = pl.ds(pl.multiple_of(n * TILE, TILE), TILE)
        keys[at, :] = key.astype(jnp.bfloat16)
        values[at, :] = value.astype(jnp.bfloat16)
        keys_t[:, at] = key.T.astype(jnp.bfloat16)
        values_t[:, at] = value.T.astype(jnp.bfloat16)
        return carry

    lax.fori_loop(0, SLABS // 2, step, 0, unroll=4)


def chunks():
    for b in range(ROWS // TILE):
        yield b * TILE, slice(b * CHUNK, (b + 1) * CHUNK)


def score_half(keys, query, scores, peak, core, place, key_core):
    for low, at in chunks():
        s = dot(keys[at, :], query[low:, :], NT) * SCALE_LOG2
        key = at.start + lax.broadcasted_iota(jnp.int32, (CHUNK, TILE), 0)
        key_at = (key // 64) * 128 + ((key % 64) // 4) * 8 + key_core * 4 + key % 4
        row = low + lax.broadcasted_iota(jnp.int32, (CHUNK, TILE), 1)
        row_at = (row // 32) * 128 + place * 8 + core * 4 + (row % 32) // 8
        near = jnp.where(key_at <= row_at, s[:, :TILE], HIDDEN_SCORE)
        scores[at, low : low + TILE] = near
        peak[:, low : low + TILE] = jnp.maximum(peak[:, low : low + TILE], fold_rows(near, jnp.max))
        if low + TILE < ROWS:
            far = s[:, TILE:]
            scores[at, low + TILE :] = far
            peak[:, low + TILE :] = jnp.maximum(peak[:, low + TILE :], fold_rows(far, jnp.max))


def forward_half(scores, weights, values_t, peak, total, attended_t):
    for low, at in chunks():
        p = jnp.exp2(scores[at, low:] - peak[0:1, low:])
        weights[at, low:] = p
        total[:, low:] += fold_rows(p, jnp.sum)
        high, rest = two_parts(p)
        v = values_t[:, at]
        attended_t[:, low:] += dot(v, high) + dot(v, rest)


def add_query_grad(low, at, keys_t, d_high, d_rest, grad_query_t):
    k = keys_t[:, at]
    grad_query_t[:, low:] += dot(k, d_high) + dot(k, d_rest)


def backward_half(query, cotangent, values, weights, inverse, delta, grad_ref, grad_peak, take_dscore):
    first = lax.broadcasted_iota(jnp.int32, (PEERS // 2, 8, WIDTH), 1) < 4
    grad_peak[...] = jnp.zeros(grad_peak.shape, jnp.float32)
    for low, at in chunks():
        grad = dot(values[at, :], cotangent[low:, :], NT)
        p = weights[at, low:] * inverse[0:1, low:]
        p_high, p_rest = two_parts(p)
        d_high, d_rest = two_parts(p * (grad - delta[0:1, low:]))
        value_grad = dot(p_high, cotangent[low:, :]) + dot(p_rest, cotangent[low:, :])
        key_grad = SCALE * (dot(d_high, query[low:, :]) + dot(d_rest, query[low:, :]))
        take_dscore(low, at, d_high, d_rest)
        both = jnp.maximum(jnp.abs(key_grad), jnp.abs(value_grad))
        grad_peak[...] = jnp.maximum(grad_peak[...], fold_rows(both, jnp.max))
        for n in range(CHUNK // 64):
            kg = key_grad[n * 64 : (n + 1) * 64].reshape(PEERS // 2, 8, WIDTH)
            vg = value_grad[n * 64 : (n + 1) * 64].reshape(PEERS // 2, 8, WIDTH)
            slab = at.start // 64 + n
            grad_ref[:, 0, slab] = jnp.where(first, kg, pltpu.roll(vg, 4, 1))
            grad_ref[:, 1, slab] = jnp.where(first, pltpu.roll(kg, 4, 1), vg)
    grad_ref[:, :, SLABS] = jnp.full((PEERS // 2, 2, 8, WIDTH), jnp.max(grad_peak[...]), jnp.float32)


def prepare_kernel(rows_ref, query, cotangent, cotangent_t):
    query[...] = rows_ref[:, 0:32, :].reshape(ROWS, WIDTH)
    cotangent[...] = rows_ref[:, 32:64, :].reshape(ROWS, WIDTH)
    cotangent_t[...] = cotangent[...].astype(jnp.float32).T


def first_kernel(
    place_ref, mine_ref, query, keys_t, values, weights, peak, total, attended_t, keys, values_t
):
    sort_half(mine_ref, keys, values, keys_t, values_t)
    peak[...] = jnp.full(peak.shape, HIDDEN_SCORE, jnp.float32)
    score_half(keys, query, weights, peak, place_ref[0], place_ref[1], place_ref[0])
    peak[...] = jnp.broadcast_to(jnp.max(peak[...], axis=0, keepdims=True), peak.shape)
    total[...] = jnp.zeros(total.shape, jnp.float32)
    attended_t[...] = jnp.zeros(attended_t.shape, jnp.float32)
    forward_half(weights, weights, values_t, peak, total, attended_t)


def second_kernel(
    place_ref,
    other_ref,
    query,
    cotangent,
    cotangent_t,
    mine_peak,
    mine_total,
    mine_attended_t,
    grad_ref,
    mine_inverse,
    delta,
    rounded_t,
    keys_t,
    dscore_high,
    dscore_rest,
    keys,
    values,
    values_t,
    scores,
    peak,
    total,
    inverse,
    attended_t,
    grad_peak,
):
    sort_half(other_ref, keys, values, keys_t, values_t)
    peak[...] = mine_peak[...]
    score_half(keys, query, scores, peak, place_ref[0], place_ref[1], 1 - place_ref[0])
    peak[...] = jnp.broadcast_to(jnp.max(peak[...], axis=0, keepdims=True), peak.shape)
    shrink = jnp.exp2(mine_peak[0:1, :] - peak[0:1, :])
    total[...] = mine_total[...] * shrink
    attended_t[...] = mine_attended_t[...] * shrink
    forward_half(scores, scores, values_t, peak, total, attended_t)
    scale = 1.0 / jnp.sum(total[...], axis=0, keepdims=True)
    inverse[...] = jnp.broadcast_to(scale, inverse.shape)
    mine_inverse[...] = jnp.broadcast_to(scale * shrink, mine_inverse.shape)
    attended = (attended_t[...] * scale).astype(jnp.bfloat16).astype(jnp.float32)
    rounded_t[...] = attended
    delta[...] = jnp.broadcast_to(jnp.sum(attended * cotangent_t[...], axis=0, keepdims=True), delta.shape)

    def keep(low, at, d_high, d_rest):
        dscore_high[at, low:] = d_high
        dscore_rest[at, low:] = d_rest

    backward_half(query, cotangent, values, scores, inverse, delta, grad_ref, grad_peak, keep)


def third_kernel(
    query,
    cotangent,
    values,
    keys_t,
    weights,
    inverse,
    delta,
    rounded_t,
    other_keys_t,
    dscore_high,
    dscore_rest,
    out_ref,
    grad_ref,
    grad_query_t,
    grad_peak,
):
    attended = rounded_t[...].T.astype(jnp.bfloat16)
    out_ref[:, 0:32, :] = attended.reshape(SLABS, 32, WIDTH)
    grad_query_t[...] = jnp.zeros(grad_query_t.shape, jnp.float32)

    def add(low, at, d_high, d_rest):
        add_query_grad(low, at, keys_t, d_high, d_rest, grad_query_t)

    backward_half(query, cotangent, values, weights, inverse, delta, grad_ref, grad_peak, add)
    for low, at in chunks():
        add_query_grad(low, at, other_keys_t, dscore_high[at, low:], dscore_rest[at, low:], grad_query_t)
    grad_query = (grad_query_t[...] * SCALE).T.astype(jnp.bfloat16)
    out_ref[:, 32:64, :] = grad_query.reshape(SLABS, 32, WIDTH)


def local_call(kernel, name, outs, scratch, passes, has_place):
    def call(*args):
        whole = pl.BlockSpec(memory_space=pltpu.VMEM)
        first = [pl.BlockSpec(memory_space=pltpu.SMEM)] if has_place else []
        return pl.pallas_call(
            kernel,
            out_shape=tuple(jax.ShapeDtypeStruct(shape, dtype) for shape, dtype in outs),
            in_specs=first + [whole] * (len(args) - len(first)),
            out_specs=(whole,) * len(outs),
            scratch_shapes=[pltpu.VMEM(shape, dtype) for shape, dtype in scratch],
            cost_estimate=pl.CostEstimate(
                flops=passes * KEYS * ROWS * WIDTH, bytes_accessed=4 << 20, transcendentals=0
            ),
            compiler_params=pltpu.CompilerParams(vmem_limit_bytes=24 << 20),
            name=name,
        )(*args)

    return call


BF, F32 = jnp.bfloat16, jnp.float32
HALF_ROWS, HALF_COLUMNS = ((KEYS // 2, WIDTH), BF), ((WIDTH, KEYS // 2), BF)
WEIGHTS, STATISTIC, ROWS_T = ((KEYS // 2, ROWS), F32), ((8, ROWS), F32), ((WIDTH, ROWS), F32)
QUERY_ROWS, SENT_ROWS = ((ROWS, WIDTH), BF), ((SLABS, 64, WIDTH), BF)
DSCORES = ((KEYS // 2, ROWS), BF)
GRADS, GRAD_PEAK = ((PEERS // 2, 2, SLABS + 1, 8, WIDTH), F32), ((8, WIDTH), F32)

prepare = local_call(prepare_kernel, "prepare", (QUERY_ROWS, QUERY_ROWS, ROWS_T), (), 1, False)
first_part = local_call(
    first_kernel,
    "first_part",
    (HALF_COLUMNS, HALF_ROWS, WEIGHTS, STATISTIC, STATISTIC, ROWS_T),
    (HALF_ROWS, HALF_COLUMNS),
    4,
    True,
)
second_part = local_call(
    second_kernel,
    "second_part",
    (GRADS, STATISTIC, STATISTIC, ROWS_T, HALF_COLUMNS, DSCORES, DSCORES),
    (HALF_ROWS, HALF_ROWS, HALF_COLUMNS, WEIGHTS, STATISTIC, STATISTIC, STATISTIC, ROWS_T, GRAD_PEAK),
    8,
    True,
)
third_part = local_call(third_kernel, "third_part", (SENT_ROWS, GRADS), (ROWS_T, GRAD_PEAK), 9, False)


def fourth(root):
    square = root.astype(jnp.float32) ** 2
    return square * square


def pack_kernel(query_ref, key_ref, value_ref, cotangent_ref, out_ref, narrow, pairs, wide_done, narrow_done):
    small = [
        pltpu.make_async_copy(source, narrow.at[n], narrow_done.at[n])
        for n, source in enumerate((key_ref, value_ref))
    ]
    for copy in small:
        copy.start()
    large = []
    for layer in range(2):
        for token in range(TOKENS):
            for n, source in enumerate((query_ref, cotangent_ref)):
                large.append(
                    pltpu.make_async_copy(
                        source.at[layer, token],
                        out_ref.at[pl.ds(layer * 8, 8), n * TOKENS + token],
                        wide_done.at[n, layer, token],
                    )
                )
    for copy in large:
        copy.start()
    for copy in small:
        copy.wait()
    for layer in range(2):
        for n in range(2):
            pairs[layer, n * TOKENS : (n + 1) * TOKENS] = narrow[n, layer].astype(jnp.float32)
        for group in range(8):
            out_ref[layer * 8 + group, 8] = pairs[layer, :, group, :].astype(jnp.bfloat16)
    for copy in large:
        copy.wait()


def pack(query, key, value, cotangent):
    far = pl.BlockSpec(memory_space=pltpu.HBM)
    by_group = (2, TOKENS, 8, GROUP, WIDTH)
    arrays = (query.reshape(by_group), key, value, cotangent.reshape(by_group))
    packed = pl.pallas_call(
        pack_kernel,
        out_shape=jax.ShapeDtypeStruct((SLABS, 9, 8, WIDTH), jnp.bfloat16),
        in_specs=[far] * 4,
        out_specs=pl.BlockSpec(memory_space=pltpu.VMEM),
        scratch_shapes=[
            pltpu.VMEM((2, 2, TOKENS, 8, WIDTH), jnp.bfloat16),
            pltpu.VMEM((2, 8, 8, WIDTH), jnp.float32),
            pltpu.SemaphoreType.DMA((2, 2, TOKENS)),
            pltpu.SemaphoreType.DMA((2,)),
        ],
        compiler_params=pltpu.CompilerParams(vmem_limit_bytes=4 << 20),
        name="pack",
    )(*[pltpu.with_memory_space_constraint(a, pltpu.HBM) for a in arrays])
    return packed.reshape(SLABS, 72, WIDTH)


def unpack_kernel(
    back_ref, attended_ref, grad_query_ref, grad_key_ref, grad_value_ref, narrow, pairs, wide_done, narrow_done
):
    copies = []
    for layer in range(2):
        for token in range(TOKENS):
            for n, target in enumerate((attended_ref, grad_query_ref)):
                copies.append(
                    pltpu.make_async_copy(
                        back_ref.at[pl.ds(layer * 8, 8), n * TOKENS + token],
                        target.at[layer, token],
                        wide_done.at[n, layer, token],
                    )
                )
    for copy in copies:
        copy.start()
    for layer in range(2):
        for group in range(8):
            pairs[layer, :, group, :] = back_ref[layer * 8 + group, 8].astype(jnp.float32)
        for n in range(2):
            narrow[n, layer] = pairs[layer, n * TOKENS : (n + 1) * TOKENS].astype(jnp.bfloat16)
    small = [
        pltpu.make_async_copy(narrow.at[n], target, narrow_done.at[n])
        for n, target in enumerate((grad_key_ref, grad_value_ref))
    ]
    for copy in small:
        copy.start()
    for copy in copies + small:
        copy.wait()


def unpack(back):
    far = pl.BlockSpec(memory_space=pltpu.HBM)
    wide = jax.ShapeDtypeStruct((2, TOKENS, 8, GROUP, WIDTH), jnp.bfloat16)
    thin = jax.ShapeDtypeStruct((2, TOKENS, 8, WIDTH), jnp.bfloat16)
    attended, grad_query, grad_key, grad_value = pl.pallas_call(
        unpack_kernel,
        out_shape=(wide, wide, thin, thin),
        in_specs=[pl.BlockSpec(memory_space=pltpu.VMEM)],
        out_specs=(far,) * 4,
        scratch_shapes=[
            pltpu.VMEM((2, 2, TOKENS, 8, WIDTH), jnp.bfloat16),
            pltpu.VMEM((2, 8, 8, WIDTH), jnp.float32),
            pltpu.SemaphoreType.DMA((2, 2, TOKENS)),
            pltpu.SemaphoreType.DMA((2,)),
        ],
        compiler_params=pltpu.CompilerParams(vmem_limit_bytes=4 << 20),
        name="unpack",
    )(back.reshape(SLABS, 9, 8, WIDTH))
    heads = (2, TOKENS, 64, WIDTH)
    return attended.reshape(heads), grad_query.reshape(heads), grad_key, grad_value


def on_device(query, key, value, cotangent):
    core = lax.axis_index("c")
    place = jnp.stack([core, lax.axis_index("y") * 4 + lax.axis_index("x")]).astype(jnp.int32)
    rows = lax.all_to_all(pack(query, key, value, cotangent), "z", 0, 0)
    slab = jnp.broadcast_to(rows[:, 64:72, :][None], (PEERS, SLABS, 8, WIDTH))
    mine = lax.all_to_all(slab, PLANE, 0, 0)
    query, cotangent, cotangent_t = prepare(rows)
    swap = [(0, 1), (1, 0)]
    halves = (PEERS // 2, 2, SLABS, 8, WIDTH)
    other = lax.ppermute(mine, "c", swap)
    keys_t, values, weights, *forward = first_part(place, mine.reshape(halves), query)
    other_grad, inverse, delta, *rest = second_part(
        place, other.reshape(halves), query, cotangent, cotangent_t, *forward
    )
    swapped = lax.ppermute(other_grad, "c", swap)
    out, mine_grad = third_part(query, cotangent, values, keys_t, weights, inverse, delta, *rest)
    total = (mine_grad + swapped).reshape(PEERS, SLABS + 1, 8, WIDTH)
    root = jnp.sqrt(jnp.sqrt(jnp.maximum(total[:, SLABS:], 1e-15)))
    root = lax.reduce_precision(root, exponent_bits=5, mantissa_bits=10)
    last = lax.broadcasted_iota(jnp.int32, total.shape, 1) == SLABS
    sent = jnp.where(last, root, total * (FULL / fourth(root))).astype(jnp.float16)
    parts = lax.all_to_all(sent, PLANE, 0, 0)
    scales = fourth(parts[:, SLABS:]) * (1.0 / FULL)
    pair_grad = jnp.sum(parts[:, :SLABS].astype(jnp.float32) * scales, axis=0).astype(jnp.bfloat16)
    back = lax.all_to_all(jnp.concatenate([out, pair_grad], axis=1), "z", 0, 0)
    return unpack(back)


def solution(mesh):
    torus = Mesh(mesh.devices.reshape(16, 4, 4, 2), AXES)
    spec = P(None, AXES, None, None)
    return jax.shard_map(
        on_device, mesh=torus, in_specs=(spec,) * 4, out_specs=(spec,) * 4, check_vma=False
    )
```

```python
import functools
import math

import jax
import jax.numpy as jnp
from jax import lax
from jax.experimental import pallas as pl
from jax.experimental.pallas import tpu as pltpu
from jax.sharding import Mesh
from jax.sharding import PartitionSpec as P

AXES = ("z", "y", "x", "c")
PLANE = ("y", "x")
SLABS, PEERS = 16, 16
TOKENS, GROUP, WIDTH = 4, 8, 128
ROWS = SLABS * TOKENS * GROUP
KEYS = 2048
CHUNK = 256
TILE = 128
HIDDEN_SCORE = -1e30
FULL = 2.0**14
SCALE = WIDTH**-0.5
SCALE_LOG2 = SCALE * math.log2(math.e)

NT = (((1,), (1,)), ((), ()))
NN = (((1,), (0,)), ((), ()))


def dot(a, b, dims=NN):
    return lax.dot_general(a, b, dims, preferred_element_type=jnp.float32)


def two_parts(value):
    high = value.astype(jnp.bfloat16)
    return high, (value - high.astype(jnp.float32)).astype(jnp.bfloat16)


def fold_rows(value, op):
    return op(value.reshape(value.shape[0] // 8, 8, value.shape[1]), axis=0)


def sort_half(half_ref, keys, values, keys_t, values_t):
    first = lax.broadcasted_iota(jnp.int32, (PEERS // 2, 8, WIDTH), 1) < 4

    def step(n, carry):
        sorted_keys, sorted_values = [], []
        for slab in range(2):
            even = half_ref[:, 0, 2 * n + slab].astype(jnp.float32)
            odd = half_ref[:, 1, 2 * n + slab].astype(jnp.float32)
            sorted_keys.append(jnp.where(first, even, pltpu.roll(odd, 4, 1)).reshape(64, WIDTH))
            sorted_values.append(jnp.where(first, pltpu.roll(even, 4, 1), odd).reshape(64, WIDTH))
        key, value = jnp.concatenate(sorted_keys, axis=0), jnp.concatenate(sorted_values, axis=0)
        at = pl.ds(pl.multiple_of(n * TILE, TILE), TILE)
        keys[at, :] = key.astype(jnp.bfloat16)
        values[at, :] = value.astype(jnp.bfloat16)
        keys_t[:, at] = key.T.astype(jnp.bfloat16)
        values_t[:, at] = value.T.astype(jnp.bfloat16)
        return carry

    lax.fori_loop(0, SLABS // 2, step, 0, unroll=4)


def chunks():
    for b in range(ROWS // TILE):
        yield b * TILE, slice(b * CHUNK, (b + 1) * CHUNK)


def score_half(keys, query, scores, peak, core, place, key_core):
    for low, at in chunks():
        s = dot(keys[at, :], query[low:, :], NT) * SCALE_LOG2
        key = at.start + lax.broadcasted_iota(jnp.int32, (CHUNK, TILE), 0)
        key_at = (key // 64) * 128 + ((key % 64) // 4) * 8 + key_core * 4 + key % 4
        row = low + lax.broadcasted_iota(jnp.int32, (CHUNK, TILE), 1)
        row_at = (row // 32) * 128 + place * 8 + core * 4 + (row % 32) // 8
        near = jnp.where(key_at <= row_at, s[:, :TILE], HIDDEN_SCORE)
        scores[at, low : low + TILE] = near
        peak[:, low : low + TILE] = jnp.maximum(peak[:, low : low + TILE], fold_rows(near, jnp.max))
        if low + TILE < ROWS:
            far = s[:, TILE:]
            scores[at, low + TILE :] = far
            peak[:, low + TILE :] = jnp.maximum(peak[:, low + TILE :], fold_rows(far, jnp.max))


def forward_half(scores, weights, values_t, peak, total, attended_t):
    for low, at in chunks():
        p = jnp.exp2(scores[at, low:] - peak[0:1, low:])
        weights[at, low:] = p
        total[:, low:] += fold_rows(p, jnp.sum)
        high, rest = two_parts(p)
        v = values_t[:, at]
        attended_t[:, low:] += dot(v, high) + dot(v, rest)


def add_query_grad(low, at, keys_t, d_high, d_rest, grad_query_t):
    k = keys_t[:, at]
    grad_query_t[:, low:] += dot(k, d_high) + dot(k, d_rest)


def backward_half(query, cotangent, values, weights, inverse, delta, grad_ref, grad_peak, take_dscore):
    first = lax.broadcasted_iota(jnp.int32, (PEERS // 2, 8, WIDTH), 1) < 4
    grad_peak[...] = jnp.zeros(grad_peak.shape, jnp.float32)
    for low, at in chunks():
        grad = dot(values[at, :], cotangent[low:, :], NT)
        p = weights[at, low:] * inverse[0:1, low:]
        p_high, p_rest = two_parts(p)
        d_high, d_rest = two_parts(p * (grad - delta[0:1, low:]))
        value_grad = dot(p_high, cotangent[low:, :]) + dot(p_rest, cotangent[low:, :])
        key_grad = SCALE * (dot(d_high, query[low:, :]) + dot(d_rest, query[low:, :]))
        take_dscore(low, at, d_high, d_rest)
        both = jnp.maximum(jnp.abs(key_grad), jnp.abs(value_grad))
        grad_peak[...] = jnp.maximum(grad_peak[...], fold_rows(both, jnp.max))
        for n in range(CHUNK // 64):
            kg = key_grad[n * 64 : (n + 1) * 64].reshape(PEERS // 2, 8, WIDTH)
            vg = value_grad[n * 64 : (n + 1) * 64].reshape(PEERS // 2, 8, WIDTH)
            slab = at.start // 64 + n
            grad_ref[:, 0, slab] = jnp.where(first, kg, pltpu.roll(vg, 4, 1))
            grad_ref[:, 1, slab] = jnp.where(first, pltpu.roll(kg, 4, 1), vg)
    grad_ref[:, :, SLABS] = jnp.full((PEERS // 2, 2, 8, WIDTH), jnp.max(grad_peak[...]), jnp.float32)


def prepare_kernel(rows_ref, query, cotangent, cotangent_t):
    query[...] = rows_ref[:, 0:32, :].reshape(ROWS, WIDTH)
    cotangent[...] = rows_ref[:, 32:64, :].reshape(ROWS, WIDTH)
    cotangent_t[...] = cotangent[...].astype(jnp.float32).T


def first_kernel(
    place_ref, mine_ref, query, keys_t, values, weights, peak, total, attended_t, keys, values_t
):
    sort_half(mine_ref, keys, values, keys_t, values_t)
    peak[...] = jnp.full(peak.shape, HIDDEN_SCORE, jnp.float32)
    score_half(keys, query, weights, peak, place_ref[0], place_ref[1], place_ref[0])
    peak[...] = jnp.broadcast_to(jnp.max(peak[...], axis=0, keepdims=True), peak.shape)
    total[...] = jnp.zeros(total.shape, jnp.float32)
    attended_t[...] = jnp.zeros(attended_t.shape, jnp.float32)
    forward_half(weights, weights, values_t, peak, total, attended_t)


def second_kernel(
    place_ref,
    other_ref,
    query,
    cotangent,
    cotangent_t,
    mine_peak,
    mine_total,
    mine_attended_t,
    grad_ref,
    mine_inverse,
    delta,
    rounded_t,
    keys_t,
    dscore_high,
    dscore_rest,
    keys,
    values,
    values_t,
    scores,
    peak,
    total,
    inverse,
    attended_t,
    grad_peak,
):
    sort_half(other_ref, keys, values, keys_t, values_t)
    peak[...] = mine_peak[...]
    score_half(keys, query, scores, peak, place_ref[0], place_ref[1], 1 - place_ref[0])
    peak[...] = jnp.broadcast_to(jnp.max(peak[...], axis=0, keepdims=True), peak.shape)
    shrink = jnp.exp2(mine_peak[0:1, :] - peak[0:1, :])
    total[...] = mine_total[...] * shrink
    attended_t[...] = mine_attended_t[...] * shrink
    forward_half(scores, scores, values_t, peak, total, attended_t)
    scale = 1.0 / jnp.sum(total[...], axis=0, keepdims=True)
    inverse[...] = jnp.broadcast_to(scale, inverse.shape)
    mine_inverse[...] = jnp.broadcast_to(scale * shrink, mine_inverse.shape)
    attended = (attended_t[...] * scale).astype(jnp.bfloat16).astype(jnp.float32)
    rounded_t[...] = attended
    delta[...] = jnp.broadcast_to(jnp.sum(attended * cotangent_t[...], axis=0, keepdims=True), delta.shape)

    def keep(low, at, d_high, d_rest):
        dscore_high[at, low:] = d_high
        dscore_rest[at, low:] = d_rest

    backward_half(query, cotangent, values, scores, inverse, delta, grad_ref, grad_peak, keep)


def third_kernel(
    query,
    cotangent,
    values,
    keys_t,
    weights,
    inverse,
    delta,
    rounded_t,
    other_keys_t,
    dscore_high,
    dscore_rest,
    out_ref,
    grad_ref,
    grad_query_t,
    grad_peak,
):
    attended = rounded_t[...].T.astype(jnp.bfloat16)
    out_ref[:, 0:32, :] = attended.reshape(SLABS, 32, WIDTH)
    grad_query_t[...] = jnp.zeros(grad_query_t.shape, jnp.float32)

    def add(low, at, d_high, d_rest):
        add_query_grad(low, at, keys_t, d_high, d_rest, grad_query_t)

    backward_half(query, cotangent, values, weights, inverse, delta, grad_ref, grad_peak, add)
    for low, at in chunks():
        add_query_grad(low, at, other_keys_t, dscore_high[at, low:], dscore_rest[at, low:], grad_query_t)
    grad_query = (grad_query_t[...] * SCALE).T.astype(jnp.bfloat16)
    out_ref[:, 32:64, :] = grad_query.reshape(SLABS, 32, WIDTH)


def local_call(kernel, name, outs, scratch, passes, has_place):
    def call(*args):
        whole = pl.BlockSpec(memory_space=pltpu.VMEM)
        first = [pl.BlockSpec(memory_space=pltpu.SMEM)] if has_place else []
        return pl.pallas_call(
            kernel,
            out_shape=tuple(jax.ShapeDtypeStruct(shape, dtype) for shape, dtype in outs),
            in_specs=first + [whole] * (len(args) - len(first)),
            out_specs=(whole,) * len(outs),
            scratch_shapes=[pltpu.VMEM(shape, dtype) for shape, dtype in scratch],
            cost_estimate=pl.CostEstimate(
                flops=passes * KEYS * ROWS * WIDTH, bytes_accessed=4 << 20, transcendentals=0
            ),
            compiler_params=pltpu.CompilerParams(vmem_limit_bytes=24 << 20),
            name=name,
        )(*args)

    return call


BF, F32 = jnp.bfloat16, jnp.float32
HALF_ROWS, HALF_COLUMNS = ((KEYS // 2, WIDTH), BF), ((WIDTH, KEYS // 2), BF)
WEIGHTS, STATISTIC, ROWS_T = ((KEYS // 2, ROWS), F32), ((8, ROWS), F32), ((WIDTH, ROWS), F32)
QUERY_ROWS, SENT_ROWS = ((ROWS, WIDTH), BF), ((SLABS, 64, WIDTH), BF)
DSCORES = ((KEYS // 2, ROWS), BF)
GRADS, GRAD_PEAK = ((PEERS // 2, 2, SLABS + 1, 8, WIDTH), F32), ((8, WIDTH), F32)

prepare = local_call(prepare_kernel, "prepare", (QUERY_ROWS, QUERY_ROWS, ROWS_T), (), 1, False)
first_part = local_call(
    first_kernel,
    "first_part",
    (HALF_COLUMNS, HALF_ROWS, WEIGHTS, STATISTIC, STATISTIC, ROWS_T),
    (HALF_ROWS, HALF_COLUMNS),
    4,
    True,
)
second_part = local_call(
    second_kernel,
    "second_part",
    (GRADS, STATISTIC, STATISTIC, ROWS_T, HALF_COLUMNS, DSCORES, DSCORES),
    (HALF_ROWS, HALF_ROWS, HALF_COLUMNS, WEIGHTS, STATISTIC, STATISTIC, STATISTIC, ROWS_T, GRAD_PEAK),
    8,
    True,
)
third_part = local_call(third_kernel, "third_part", (SENT_ROWS, GRADS), (ROWS_T, GRAD_PEAK), 9, False)


def fourth(root):
    square = root.astype(jnp.float32) ** 2
    return square * square


def pack_kernel(query_ref, key_ref, value_ref, cotangent_ref, out_ref, narrow, pairs, wide_done, narrow_done):
    small = [
        pltpu.make_async_copy(source, narrow.at[n], narrow_done.at[n])
        for n, source in enumerate((key_ref, value_ref))
    ]
    for copy in small:
        copy.start()
    large = []
    for layer in range(2):
        for token in range(TOKENS):
            for n, source in enumerate((query_ref, cotangent_ref)):
                large.append(
                    pltpu.make_async_copy(
                        source.at[layer, token],
                        out_ref.at[pl.ds(layer * 8, 8), n * TOKENS + token],
                        wide_done.at[n, layer, token],
                    )
                )
    for copy in large:
        copy.start()
    for copy in small:
        copy.wait()
    for layer in range(2):
        for n in range(2):
            pairs[layer, n * TOKENS : (n + 1) * TOKENS] = narrow[n, layer].astype(jnp.float32)
        for group in range(8):
            out_ref[layer * 8 + group, 8] = pairs[layer, :, group, :].astype(jnp.bfloat16)
    for copy in large:
        copy.wait()


def pack(query, key, value, cotangent):
    far = pl.BlockSpec(memory_space=pltpu.HBM)
    by_group = (2, TOKENS, 8, GROUP, WIDTH)
    arrays = (query.reshape(by_group), key, value, cotangent.reshape(by_group))
    packed = pl.pallas_call(
        pack_kernel,
        out_shape=jax.ShapeDtypeStruct((SLABS, 9, 8, WIDTH), jnp.bfloat16),
        in_specs=[far] * 4,
        out_specs=pl.BlockSpec(memory_space=pltpu.VMEM),
        scratch_shapes=[
            pltpu.VMEM((2, 2, TOKENS, 8, WIDTH), jnp.bfloat16),
            pltpu.VMEM((2, 8, 8, WIDTH), jnp.float32),
            pltpu.SemaphoreType.DMA((2, 2, TOKENS)),
            pltpu.SemaphoreType.DMA((2,)),
        ],
        compiler_params=pltpu.CompilerParams(vmem_limit_bytes=4 << 20),
        name="pack",
    )(*[pltpu.with_memory_space_constraint(a, pltpu.HBM) for a in arrays])
    return packed.reshape(SLABS, 72, WIDTH)


def unpack_kernel(
    back_ref, attended_ref, grad_query_ref, grad_key_ref, grad_value_ref, narrow, pairs, wide_done, narrow_done
):
    copies = []
    for layer in range(2):
        for token in range(TOKENS):
            for n, target in enumerate((attended_ref, grad_query_ref)):
                copies.append(
                    pltpu.make_async_copy(
                        back_ref.at[pl.ds(layer * 8, 8), n * TOKENS + token],
                        target.at[layer, token],
                        wide_done.at[n, layer, token],
                    )
                )
    for copy in copies:
        copy.start()
    for layer in range(2):
        for group in range(8):
            pairs[layer, :, group, :] = back_ref[layer * 8 + group, 8].astype(jnp.float32)
        for n in range(2):
            narrow[n, layer] = pairs[layer, n * TOKENS : (n + 1) * TOKENS].astype(jnp.bfloat16)
    small = [
        pltpu.make_async_copy(narrow.at[n], target, narrow_done.at[n])
        for n, target in enumerate((grad_key_ref, grad_value_ref))
    ]
    for copy in small:
        copy.start()
    for copy in copies + small:
        copy.wait()


def unpack(back):
    far = pl.BlockSpec(memory_space=pltpu.HBM)
    wide = jax.ShapeDtypeStruct((2, TOKENS, 8, GROUP, WIDTH), jnp.bfloat16)
    thin = jax.ShapeDtypeStruct((2, TOKENS, 8, WIDTH), jnp.bfloat16)
    attended, grad_query, grad_key, grad_value = pl.pallas_call(
        unpack_kernel,
        out_shape=(wide, wide, thin, thin),
        in_specs=[pl.BlockSpec(memory_space=pltpu.VMEM)],
        out_specs=(far,) * 4,
        scratch_shapes=[
            pltpu.VMEM((2, 2, TOKENS, 8, WIDTH), jnp.bfloat16),
            pltpu.VMEM((2, 8, 8, WIDTH), jnp.float32),
            pltpu.SemaphoreType.DMA((2, 2, TOKENS)),
            pltpu.SemaphoreType.DMA((2,)),
        ],
        compiler_params=pltpu.CompilerParams(vmem_limit_bytes=4 << 20),
        name="unpack",
    )(back.reshape(SLABS, 9, 8, WIDTH))
    heads = (2, TOKENS, 64, WIDTH)
    return attended.reshape(heads), grad_query.reshape(heads), grad_key, grad_value


def on_device(query, key, value, cotangent):
    core = lax.axis_index("c")
    place = jnp.stack([core, lax.axis_index("y") * 4 + lax.axis_index("x")]).astype(jnp.int32)
    rows = lax.all_to_all(pack(query, key, value, cotangent), "z", 0, 0)
    slab = jnp.broadcast_to(rows[:, 64:72, :][None], (PEERS, SLABS, 8, WIDTH))
    mine = lax.all_to_all(slab, PLANE, 0, 0)
    query, cotangent, cotangent_t = prepare(rows)
    swap = [(0, 1), (1, 0)]
    halves = (PEERS // 2, 2, SLABS, 8, WIDTH)
    other = lax.ppermute(mine, "c", swap)
    keys_t, values, weights, *forward = first_part(place, mine.reshape(halves), query)
    other_grad, inverse, delta, *rest = second_part(
        place, other.reshape(halves), query, cotangent, cotangent_t, *forward
    )
    swapped = lax.ppermute(other_grad, "c", swap)
    out, mine_grad = third_part(query, cotangent, values, keys_t, weights, inverse, delta, *rest)
    blocks = (PEERS, SLABS + 1, 8, WIDTH)
    mine_grad, swapped = mine_grad.reshape(blocks), swapped.reshape(blocks)
    bound = mine_grad[:, SLABS:] + swapped[:, SLABS:]
    root = jnp.sqrt(jnp.sqrt(jnp.maximum(bound, 1e-15)))
    root = lax.reduce_precision(root, exponent_bits=5, mantissa_bits=10)
    last = lax.broadcasted_iota(jnp.int32, blocks, 1) == SLABS
    sent = jnp.where(last, root, (mine_grad + swapped) * (FULL / fourth(root))).astype(jnp.float16)
    parts = lax.all_to_all(sent, PLANE, 0, 0)
    scales = fourth(parts[:, SLABS:]) * (1.0 / FULL)
    pair_grad = jnp.sum(parts[:, :SLABS].astype(jnp.float32) * scales, axis=0).astype(jnp.bfloat16)
    back = lax.all_to_all(jnp.concatenate([out, pair_grad], axis=1), "z", 0, 0)
    return unpack(back)


def solution(mesh):
    torus = Mesh(mesh.devices.reshape(16, 4, 4, 2), AXES)
    spec = P(None, AXES, None, None)
    return jax.shard_map(
        on_device, mesh=torus, in_specs=(spec,) * 4, out_specs=(spec,) * 4, check_vma=False
    )
```

```python
import functools
import math

import jax
import jax.numpy as jnp
from jax import lax
from jax.experimental import pallas as pl
from jax.experimental.pallas import tpu as pltpu
from jax.sharding import Mesh
from jax.sharding import PartitionSpec as P

AXES = ("z", "y", "x", "c")
PLANE = ("y", "x")
SLABS, PEERS = 16, 16
TOKENS, GROUP, WIDTH = 4, 8, 128
ROWS = SLABS * TOKENS * GROUP
KEYS = 2048
CHUNK = 256
TILE = 128
HIDDEN_SCORE = -1e30
FULL = 2.0**14
SCALE = WIDTH**-0.5
SCALE_LOG2 = SCALE * math.log2(math.e)

NT = (((1,), (1,)), ((), ()))
NN = (((1,), (0,)), ((), ()))


def dot(a, b, dims=NN):
    return lax.dot_general(a, b, dims, preferred_element_type=jnp.float32)


def two_parts(value):
    high = value.astype(jnp.bfloat16)
    return high, (value - high.astype(jnp.float32)).astype(jnp.bfloat16)


def fold_rows(value, op):
    return op(value.reshape(value.shape[0] // 8, 8, value.shape[1]), axis=0)


def sort_half(half_ref, keys, values, keys_t, values_t):
    first = lax.broadcasted_iota(jnp.int32, (PEERS // 2, 8, WIDTH), 1) < 4

    def step(n, carry):
        sorted_keys, sorted_values = [], []
        for slab in range(2):
            even = half_ref[:, 0, 2 * n + slab].astype(jnp.float32)
            odd = half_ref[:, 1, 2 * n + slab].astype(jnp.float32)
            sorted_keys.append(jnp.where(first, even, pltpu.roll(odd, 4, 1)).reshape(64, WIDTH))
            sorted_values.append(jnp.where(first, pltpu.roll(even, 4, 1), odd).reshape(64, WIDTH))
        key, value = jnp.concatenate(sorted_keys, axis=0), jnp.concatenate(sorted_values, axis=0)
        at = pl.ds(pl.multiple_of(n * TILE, TILE), TILE)
        keys[at, :] = key.astype(jnp.bfloat16)
        values[at, :] = value.astype(jnp.bfloat16)
        keys_t[:, at] = key.T.astype(jnp.bfloat16)
        values_t[:, at] = value.T.astype(jnp.bfloat16)
        return carry

    lax.fori_loop(0, SLABS // 2, step, 0, unroll=4)


def chunks():
    for b in range(ROWS // TILE):
        yield b * TILE, slice(b * CHUNK, (b + 1) * CHUNK)


def score_half(keys, query, scores, peak, core, place, key_core):
    for low, at in chunks():
        s = dot(keys[at, :], query[low:, :], NT) * SCALE_LOG2
        key = at.start + lax.broadcasted_iota(jnp.int32, (CHUNK, TILE), 0)
        key_at = (key // 64) * 128 + ((key % 64) // 4) * 8 + key_core * 4 + key % 4
        row = low + lax.broadcasted_iota(jnp.int32, (CHUNK, TILE), 1)
        row_at = (row // 32) * 128 + place * 8 + core * 4 + (row % 32) // 8
        near = jnp.where(key_at <= row_at, s[:, :TILE], HIDDEN_SCORE)
        scores[at, low : low + TILE] = near
        peak[:, low : low + TILE] = jnp.maximum(peak[:, low : low + TILE], fold_rows(near, jnp.max))
        if low + TILE < ROWS:
            far = s[:, TILE:]
            scores[at, low + TILE :] = far
            peak[:, low + TILE :] = jnp.maximum(peak[:, low + TILE :], fold_rows(far, jnp.max))


def forward_half(scores, weights, values_t, peak, total, attended_t):
    for low, at in chunks():
        p = jnp.exp2(scores[at, low:] - peak[0:1, low:])
        weights[at, low:] = p
        total[:, low:] += fold_rows(p, jnp.sum)
        high, rest = two_parts(p)
        v = values_t[:, at]
        attended_t[:, low:] += dot(v, high) + dot(v, rest)


def add_query_grad(low, at, keys_t, d_high, d_rest, grad_query_t):
    k = keys_t[:, at]
    grad_query_t[:, low:] += dot(k, d_high) + dot(k, d_rest)


def backward_half(query, cotangent, values, weights, inverse, delta, grad_ref, grad_peak, take_dscore):
    first = lax.broadcasted_iota(jnp.int32, (PEERS // 2, 8, WIDTH), 1) < 4
    grad_peak[...] = jnp.zeros(grad_peak.shape, jnp.float32)
    for low, at in chunks():
        grad = dot(values[at, :], cotangent[low:, :], NT)
        p = weights[at, low:] * inverse[0:1, low:]
        p_high, p_rest = two_parts(p)
        d_high, d_rest = two_parts(p * (grad - delta[0:1, low:]))
        value_grad = dot(p_high, cotangent[low:, :]) + dot(p_rest, cotangent[low:, :])
        key_grad = SCALE * (dot(d_high, query[low:, :]) + dot(d_rest, query[low:, :]))
        take_dscore(low, at, d_high, d_rest)
        both = jnp.maximum(jnp.abs(key_grad), jnp.abs(value_grad))
        grad_peak[...] = jnp.maximum(grad_peak[...], fold_rows(both, jnp.max))
        for n in range(CHUNK // 64):
            kg = key_grad[n * 64 : (n + 1) * 64].reshape(PEERS // 2, 8, WIDTH)
            vg = value_grad[n * 64 : (n + 1) * 64].reshape(PEERS // 2, 8, WIDTH)
            slab = at.start // 64 + n
            grad_ref[:, 0, slab] = jnp.where(first, kg, pltpu.roll(vg, 4, 1))
            grad_ref[:, 1, slab] = jnp.where(first, pltpu.roll(kg, 4, 1), vg)
    grad_ref[:, :, SLABS] = jnp.full((PEERS // 2, 2, 8, WIDTH), jnp.max(grad_peak[...]), jnp.float32)


def first_kernel(
    place_ref, rows_ref, mine_ref, query, cotangent, cotangent_t, keys, values, keys_t, values_t, scores, peak
):
    query[...] = rows_ref[:, 0:32, :].reshape(ROWS, WIDTH)
    cotangent[...] = rows_ref[:, 32:64, :].reshape(ROWS, WIDTH)
    sort_half(mine_ref, keys, values, keys_t, values_t)
    cotangent_t[...] = cotangent[...].astype(jnp.float32).T
    peak[...] = jnp.full(peak.shape, HIDDEN_SCORE, jnp.float32)
    score_half(keys, query, scores, peak, place_ref[0], place_ref[1], place_ref[0])


def second_kernel(
    place_ref,
    other_ref,
    query,
    cotangent,
    cotangent_t,
    mine_values_t,
    mine_scores,
    mine_peak,
    grad_ref,
    mine_weights,
    inverse,
    delta,
    rounded_t,
    keys_t,
    dscore_high,
    dscore_rest,
    keys,
    values,
    values_t,
    scores,
    peak,
    total,
    attended_t,
    grad_peak,
):
    sort_half(other_ref, keys, values, keys_t, values_t)
    peak[...] = mine_peak[...]
    score_half(keys, query, scores, peak, place_ref[0], place_ref[1], 1 - place_ref[0])
    peak[...] = jnp.broadcast_to(jnp.max(peak[...], axis=0, keepdims=True), peak.shape)
    total[...] = jnp.zeros(total.shape, jnp.float32)
    attended_t[...] = jnp.zeros(attended_t.shape, jnp.float32)
    forward_half(mine_scores, mine_weights, mine_values_t, peak, total, attended_t)
    forward_half(scores, scores, values_t, peak, total, attended_t)
    scale = 1.0 / jnp.sum(total[...], axis=0, keepdims=True)
    inverse[...] = jnp.broadcast_to(scale, inverse.shape)
    attended = (attended_t[...] * scale).astype(jnp.bfloat16).astype(jnp.float32)
    rounded_t[...] = attended
    delta[...] = jnp.broadcast_to(jnp.sum(attended * cotangent_t[...], axis=0, keepdims=True), delta.shape)

    def keep(low, at, d_high, d_rest):
        dscore_high[at, low:] = d_high
        dscore_rest[at, low:] = d_rest

    backward_half(query, cotangent, values, scores, inverse, delta, grad_ref, grad_peak, keep)


def third_kernel(
    query,
    cotangent,
    values,
    keys_t,
    weights,
    inverse,
    delta,
    rounded_t,
    other_keys_t,
    dscore_high,
    dscore_rest,
    out_ref,
    grad_ref,
    grad_query_t,
    grad_peak,
):
    attended = rounded_t[...].T.astype(jnp.bfloat16)
    out_ref[:, 0:32, :] = attended.reshape(SLABS, 32, WIDTH)
    grad_query_t[...] = jnp.zeros(grad_query_t.shape, jnp.float32)

    def add(low, at, d_high, d_rest):
        add_query_grad(low, at, keys_t, d_high, d_rest, grad_query_t)

    backward_half(query, cotangent, values, weights, inverse, delta, grad_ref, grad_peak, add)
    for low, at in chunks():
        add_query_grad(low, at, other_keys_t, dscore_high[at, low:], dscore_rest[at, low:], grad_query_t)
    grad_query = (grad_query_t[...] * SCALE).T.astype(jnp.bfloat16)
    out_ref[:, 32:64, :] = grad_query.reshape(SLABS, 32, WIDTH)


HOLD_NS = 3000


def join_kernel(place_ref, rows_ref, grads_ref, out_ref):
    out_ref[:, 0:64, :] = rows_ref[...]
    out_ref[:, 64:72, :] = grads_ref[...]

    @pl.when(place_ref[0] == 1)
    def _():
        pl.delay(HOLD_NS)


def local_call(kernel, name, outs, scratch, passes, has_place):
    def call(*args):
        whole = pl.BlockSpec(memory_space=pltpu.VMEM)
        first = [pl.BlockSpec(memory_space=pltpu.SMEM)] if has_place else []
        return pl.pallas_call(
            kernel,
            out_shape=tuple(jax.ShapeDtypeStruct(shape, dtype) for shape, dtype in outs),
            in_specs=first + [whole] * (len(args) - len(first)),
            out_specs=(whole,) * len(outs),
            scratch_shapes=[pltpu.VMEM(shape, dtype) for shape, dtype in scratch],
            cost_estimate=pl.CostEstimate(
                flops=passes * KEYS * ROWS * WIDTH, bytes_accessed=4 << 20, transcendentals=0
            ),
            compiler_params=pltpu.CompilerParams(vmem_limit_bytes=24 << 20),
            name=name,
        )(*args)

    return call


BF, F32 = jnp.bfloat16, jnp.float32
HALF_ROWS, HALF_COLUMNS = ((KEYS // 2, WIDTH), BF), ((WIDTH, KEYS // 2), BF)
WEIGHTS, STATISTIC, ROWS_T = ((KEYS // 2, ROWS), F32), ((8, ROWS), F32), ((WIDTH, ROWS), F32)
QUERY_ROWS, SENT_ROWS = ((ROWS, WIDTH), BF), ((SLABS, 64, WIDTH), BF)
DSCORES = ((KEYS // 2, ROWS), BF)
GRADS, GRAD_PEAK = ((PEERS // 2, 2, SLABS + 1, 8, WIDTH), F32), ((8, WIDTH), F32)

first_part = local_call(
    first_kernel,
    "first_part",
    (QUERY_ROWS, QUERY_ROWS, ROWS_T, HALF_ROWS, HALF_ROWS, HALF_COLUMNS, HALF_COLUMNS, WEIGHTS, STATISTIC),
    (),
    2,
    True,
)
second_part = local_call(
    second_kernel,
    "second_part",
    (GRADS, WEIGHTS, STATISTIC, STATISTIC, ROWS_T, HALF_COLUMNS, DSCORES, DSCORES),
    (HALF_ROWS, HALF_ROWS, HALF_COLUMNS, WEIGHTS, STATISTIC, STATISTIC, ROWS_T, GRAD_PEAK),
    10,
    True,
)
join = local_call(join_kernel, "join", (((SLABS, 72, WIDTH), BF),), (), 1, True)
third_part = local_call(third_kernel, "third_part", (SENT_ROWS, GRADS), (ROWS_T, GRAD_PEAK), 9, False)


def fourth(root):
    square = root.astype(jnp.float32) ** 2
    return square * square


def pack_kernel(query_ref, key_ref, value_ref, cotangent_ref, out_ref, narrow, pairs, wide_done, narrow_done):
    small = [
        pltpu.make_async_copy(source, narrow.at[n], narrow_done.at[n])
        for n, source in enumerate((key_ref, value_ref))
    ]
    for copy in small:
        copy.start()
    large = []
    for layer in range(2):
        for token in range(TOKENS):
            for n, source in enumerate((query_ref, cotangent_ref)):
                large.append(
                    pltpu.make_async_copy(
                        source.at[layer, token],
                        out_ref.at[pl.ds(layer * 8, 8), n * TOKENS + token],
                        wide_done.at[n, layer, token],
                    )
                )
    for copy in large:
        copy.start()
    for copy in small:
        copy.wait()
    for layer in range(2):
        for n in range(2):
            pairs[layer, n * TOKENS : (n + 1) * TOKENS] = narrow[n, layer].astype(jnp.float32)
        for group in range(8):
            out_ref[layer * 8 + group, 8] = pairs[layer, :, group, :].astype(jnp.bfloat16)
    for copy in large:
        copy.wait()


def pack(query, key, value, cotangent):
    far = pl.BlockSpec(memory_space=pltpu.HBM)
    by_group = (2, TOKENS, 8, GROUP, WIDTH)
    arrays = (query.reshape(by_group), key, value, cotangent.reshape(by_group))
    packed = pl.pallas_call(
        pack_kernel,
        out_shape=jax.ShapeDtypeStruct((SLABS, 9, 8, WIDTH), jnp.bfloat16),
        in_specs=[far] * 4,
        out_specs=pl.BlockSpec(memory_space=pltpu.VMEM),
        scratch_shapes=[
            pltpu.VMEM((2, 2, TOKENS, 8, WIDTH), jnp.bfloat16),
            pltpu.VMEM((2, 8, 8, WIDTH), jnp.float32),
            pltpu.SemaphoreType.DMA((2, 2, TOKENS)),
            pltpu.SemaphoreType.DMA((2,)),
        ],
        compiler_params=pltpu.CompilerParams(vmem_limit_bytes=4 << 20),
        name="pack",
    )(*[pltpu.with_memory_space_constraint(a, pltpu.HBM) for a in arrays])
    return packed.reshape(SLABS, 72, WIDTH)


def unpack_kernel(
    back_ref, attended_ref, grad_query_ref, grad_key_ref, grad_value_ref, narrow, pairs, wide_done, narrow_done
):
    copies = []
    for layer in range(2):
        for token in range(TOKENS):
            for n, target in enumerate((attended_ref, grad_query_ref)):
                copies.append(
                    pltpu.make_async_copy(
                        back_ref.at[pl.ds(layer * 8, 8), n * TOKENS + token],
                        target.at[layer, token],
                        wide_done.at[n, layer, token],
                    )
                )
    for copy in copies:
        copy.start()
    for layer in range(2):
        for group in range(8):
            pairs[layer, :, group, :] = back_ref[layer * 8 + group, 8].astype(jnp.float32)
        for n in range(2):
            narrow[n, layer] = pairs[layer, n * TOKENS : (n + 1) * TOKENS].astype(jnp.bfloat16)
    small = [
        pltpu.make_async_copy(narrow.at[n], target, narrow_done.at[n])
        for n, target in enumerate((grad_key_ref, grad_value_ref))
    ]
    for copy in small:
        copy.start()
    for copy in copies + small:
        copy.wait()


def unpack(back):
    far = pl.BlockSpec(memory_space=pltpu.HBM)
    wide = jax.ShapeDtypeStruct((2, TOKENS, 8, GROUP, WIDTH), jnp.bfloat16)
    thin = jax.ShapeDtypeStruct((2, TOKENS, 8, WIDTH), jnp.bfloat16)
    attended, grad_query, grad_key, grad_value = pl.pallas_call(
        unpack_kernel,
        out_shape=(wide, wide, thin, thin),
        in_specs=[pl.BlockSpec(memory_space=pltpu.VMEM)],
        out_specs=(far,) * 4,
        scratch_shapes=[
            pltpu.VMEM((2, 2, TOKENS, 8, WIDTH), jnp.bfloat16),
            pltpu.VMEM((2, 8, 8, WIDTH), jnp.float32),
            pltpu.SemaphoreType.DMA((2, 2, TOKENS)),
            pltpu.SemaphoreType.DMA((2,)),
        ],
        compiler_params=pltpu.CompilerParams(vmem_limit_bytes=4 << 20),
        name="unpack",
    )(back.reshape(SLABS, 9, 8, WIDTH))
    heads = (2, TOKENS, 64, WIDTH)
    return attended.reshape(heads), grad_query.reshape(heads), grad_key, grad_value


def on_device(query, key, value, cotangent):
    core = lax.axis_index("c")
    place = jnp.stack([core, lax.axis_index("y") * 4 + lax.axis_index("x")]).astype(jnp.int32)
    rows = lax.all_to_all(pack(query, key, value, cotangent), "z", 0, 0)
    slab = jnp.broadcast_to(rows[:, 64:72, :][None], (PEERS, SLABS, 8, WIDTH))
    mine = lax.all_to_all(slab, PLANE, 0, 0)
    swap = [(0, 1), (1, 0)]
    halves = (PEERS // 2, 2, SLABS, 8, WIDTH)
    other = lax.ppermute(mine, "c", swap)
    query, cotangent, cotangent_t, keys, values, keys_t, values_t, scores, peak = first_part(
        place, rows, mine.reshape(halves)
    )
    other_grad, weights, inverse, delta, *rest = second_part(
        place, other.reshape(halves), query, cotangent, cotangent_t, values_t, scores, peak
    )
    swapped = lax.ppermute(other_grad, "c", swap)
    out, mine_grad = third_part(query, cotangent, values, keys_t, weights, inverse, delta, *rest)
    total = (mine_grad + swapped).reshape(PEERS, SLABS + 1, 8, WIDTH)
    root = jnp.sqrt(jnp.sqrt(jnp.maximum(total[:, SLABS:], 1e-15)))
    root = lax.reduce_precision(root, exponent_bits=5, mantissa_bits=10)
    last = lax.broadcasted_iota(jnp.int32, total.shape, 1) == SLABS
    sent = jnp.where(last, root, total * (FULL / fourth(root))).astype(jnp.float16)
    parts = lax.all_to_all(sent, PLANE, 0, 0)
    scales = fourth(parts[:, SLABS:]) * (1.0 / FULL)
    pair_grad = jnp.sum(parts[:, :SLABS].astype(jnp.float32) * scales, axis=0).astype(jnp.bfloat16)
    back = lax.all_to_all(join(place, out, pair_grad)[0], "z", 0, 0)
    return unpack(back)


def solution(mesh):
    torus = Mesh(mesh.devices.reshape(16, 4, 4, 2), AXES)
    spec = P(None, AXES, None, None)
    return jax.shard_map(
        on_device, mesh=torus, in_specs=(spec,) * 4, out_specs=(spec,) * 4, check_vma=False
    )
```
